128 devices in a mesh: frame: 16 (over x, z), row: 8 (over y, core).
Axes of the slice: x: 4, y: 4, z: 4, core: 2. Of those that a mesh axis runs over, the one named last changes fastest.
Arguments:
- latent: bfloat16 [16, 32, 160, 384], P('frame', 'row'), may hold values from -6 to 6
- first_gain: float32 [384], replicated, may hold values from 0.1 to 1.9
- first_weight: bfloat16 [3, 3, 3, 384, 384], replicated, may hold values from -0.0625 to 0.0625
- first_bias: float32 [384], replicated, may hold values from -3 to 3
- second_gain: float32 [384], replicated, may hold values from 0.1 to 1.9
- second_weight: bfloat16 [3, 3, 3, 384, 384], replicated, may hold values from -0.0625 to 0.0625
- second_bias: float32 [384], replicated, may hold values from -3 to 3
- attend_gain: float32 [384], replicated, may hold values from 0.1 to 1.9
- project_weight: bfloat16 [384, 1152], replicated, may hold values from -0.4375 to 0.4375
- project_bias: float32 [1152], replicated, may hold values from -100 to 100
- output_weight: bfloat16 [384, 384], replicated, may hold values from -0.3125 to 0.3125
- output_bias: float32 [384], replicated, may hold values from -3 to 3
- temporal_weight: bfloat16 [3, 384, 768], replicated, may hold values from -0.1875 to 0.1875
- temporal_bias: float32 [768], replicated, may hold values from -3 to 3
- upscale_weight: bfloat16 [3, 3, 384, 192], replicated, may hold values from -0.109375 to 0.109375
- upscale_bias: float32 [192], replicated, may hold values from -3 to 3
Outputs:
- upscaled: bfloat16 [32, 64, 61440], P('frame', 'row')
The draws below stay inside these ranges and needn't reach their ends.
All inputs are finite; a program needn't handle non-finite values.
Results may differ from the reference program's by a relative error of at most 0.014.
The reference program's roundings to bfloat16 on the way count: a program that leaves them out, or rounds other values in their place, can miss the bound.
Values may be sent and summed in bfloat16 or wider, within the bound.
No kernel may reach another device: no remote copies, remote signals or barrier semaphores. Data moves between devices by JAX's collectives and lax.ppermute only.
A program may use at most 128 MiB of HBM per device.

```python
import jax
import jax.numpy as jnp
from jax import lax

C = 384
CU = 192
W = 160
H = 32
FRAMES = 16


def draw_project_bias(key, part):
    first_key = jax.random.fold_in(jax.random.fold_in(key, 17), 0)
    modest = jax.random.uniform(first_key, (3 * C,), jnp.float32, -0.5, 0.5)
    return modest


def steps_of(key, dims, shards, smallest, top_value):
    loudness = 1.0
    for dim, shards_of in shards:
        steps = jax.random.uniform(jax.random.fold_in(jax.random.fold_in(key, 6), dim), (shards_of,), jnp.float32, smallest / len(shards), top_value / len(shards))
        loudness = loudness * jnp.repeat(jnp.exp(steps), dims[dim] // shards_of).reshape((-1,) + (1,) * (len(dims) - 1 - dim))
    return loudness


def bell_draw(own_key, shape, spread, limit, shards=(), dtype=jnp.bfloat16):
    factor_of = steps_of(own_key, shape, shards, -0.22, 0.18) if shards else 1.0
    array = jax.random.normal(own_key, shape, jnp.float32) * spread * factor_of
    return jnp.minimum(jnp.maximum(array, -limit), limit).astype(dtype)


def setup_inputs(seed: int = 0) -> dict:
    streams_of = jax.random.split(jax.random.key(seed), 17)
    latent = bell_draw(streams_of[0], (FRAMES, H, W, C), 1.0, 6.0, ((0, 16), (1, 8)))
    first_gain = jnp.clip(1.0 + 0.18 * jax.random.normal(streams_of[1], (C,), jnp.float32), 0.1, 1.9)
    first_weight = bell_draw(streams_of[2], (3, 3, 3, C, C), (27 * C) ** -0.5, 0.0625)
    first_bias = bell_draw(streams_of[3], (C,), 0.5, 3.0, (), jnp.float32)
    second_gain = jnp.clip(1.0 + 0.18 * jax.random.normal(streams_of[4], (C,), jnp.float32), 0.1, 1.9)
    second_weight = bell_draw(streams_of[5], (3, 3, 3, C, C), (27 * C) ** -0.5, 0.0625)
    second_bias = bell_draw(streams_of[6], (C,), 0.5, 3.0, (), jnp.float32)
    attend_gain = jnp.clip(1.0 + 0.18 * jax.random.normal(streams_of[7], (C,), jnp.float32), 0.1, 1.9)
    project_weight = bell_draw(streams_of[8], (C, 3 * C), (C // 2) ** -0.5, 0.4375)
    project_bias = draw_project_bias(jax.random.fold_in(streams_of[16], 71), 0)
    output_weight = bell_draw(streams_of[10], (C, C), C ** -0.5, 0.3125)
    output_bias = bell_draw(streams_of[11], (C,), 0.5, 3.0, (), jnp.float32)
    temporal_weight = bell_draw(streams_of[12], (3, C, 2 * C), (3 * C) ** -0.5, 0.1875)
    temporal_bias = bell_draw(streams_of[13], (2 * C,), 0.5, 3.0, (), jnp.float32)
    upscale_weight = bell_draw(streams_of[14], (3, 3, C, CU), (9 * C) ** -0.5, 0.109375)
    upscale_bias = bell_draw(streams_of[15], (CU,), 0.5, 3.0, (), jnp.float32)
    return {"latent": latent, "first_gain": first_gain, "first_weight": first_weight, "first_bias": first_bias, "second_gain": second_gain, "second_weight": second_weight, "second_bias": second_bias, "attend_gain": attend_gain, "project_weight": project_weight, "project_bias": project_bias, "output_weight": output_weight, "output_bias": output_bias, "temporal_weight": temporal_weight, "temporal_bias": temporal_bias, "upscale_weight": upscale_weight, "upscale_bias": upscale_bias}


epsilon = 1e-06

def normed(values, scaling):
    return values * lax.rsqrt(lax.optimization_barrier(jnp.mean(values * values, axis=-1, keepdims=True)) + epsilon) * scaling

def causal_conv(source, weight, biases):
    frames, height, columns, channels = source.shape
    padded = jnp.pad(source, ((2, 0), (1, 1), (1, 1), (0, 0)))
    summed = jnp.zeros((frames * height * columns, weight.shape[-1]), jnp.float32)
    for tap_time in range(3):
        for tap_row in range(3):
            for tap_col in range(3):
                window = padded[tap_time:tap_time + frames, tap_row:tap_row + height, tap_col:tap_col + columns]
                summed = summed + jnp.dot(window.reshape(-1, channels), weight[tap_time, tap_row, tap_col], preferred_element_type=jnp.float32)
    return (summed + biases).reshape(frames, height, columns, -1)

def reference(latent, first_gain, first_weight, first_bias, second_gain, second_weight, second_bias, attend_gain, project_weight, project_bias, output_weight, output_bias, temporal_weight, temporal_bias, upscale_weight, upscale_bias):
    source = latent.astype(jnp.float32)
    first_act = jax.nn.silu(normed(source, first_gain)).astype(jnp.bfloat16)
    hidden_one = causal_conv(first_act, first_weight, first_bias)
    second_act = jax.nn.silu(normed(hidden_one, second_gain)).astype(jnp.bfloat16)
    hidden_two = causal_conv(second_act, second_weight, second_bias)
    blocked = (source + hidden_two).astype(jnp.bfloat16)

    def attend(frame_rows):
        flat_rows = frame_rows.reshape(-1, C).astype(jnp.float32)
        normal_rows = normed(flat_rows, attend_gain).astype(jnp.bfloat16)
        triple = jnp.dot(normal_rows, project_weight, preferred_element_type=jnp.float32) + project_bias
        queries = triple[:, :C].astype(jnp.bfloat16)
        keys_all = triple[:, C:2 * C].astype(jnp.bfloat16)
        values_all = triple[:, 2 * C:].astype(jnp.bfloat16)
        scores = jnp.dot(queries, keys_all.T, preferred_element_type=jnp.float32) * C ** (-0.5)
        row_peak = lax.optimization_barrier(jnp.max(scores, axis=-1, keepdims=True))
        exponent = jnp.exp(scores - row_peak)
        weights = exponent.astype(jnp.bfloat16)
        attended = (jnp.dot(weights, values_all, preferred_element_type=jnp.float32) / lax.optimization_barrier(jnp.sum(exponent, axis=-1, keepdims=True))).astype(jnp.bfloat16)
        mixed_rows = flat_rows + jnp.dot(attended, output_weight, preferred_element_type=jnp.float32) + output_bias
        return mixed_rows.astype(jnp.bfloat16).reshape(H, W, C)
    mixed = lax.map(attend, blocked)
    padded_mix = jnp.pad(mixed, ((2, 0), (0, 0), (0, 0), (0, 0)))
    stacked = jnp.concatenate([padded_mix[0:FRAMES], padded_mix[1:FRAMES + 1], padded_mix[2:FRAMES + 2]], axis=-1)
    doubled = jnp.dot(stacked.reshape(-1, 3 * C), temporal_weight.reshape(3 * C, 2 * C), preferred_element_type=jnp.float32) + temporal_bias
    doubled = doubled.astype(jnp.bfloat16).reshape(FRAMES, H, W, 2 * C)
    expanded = jnp.stack([doubled[..., :C], doubled[..., C:]], axis=1).reshape(2 * FRAMES, H, W, C)

    def upscale_frame(frame_rows):
        tall_rows = jnp.repeat(jnp.repeat(frame_rows, 2, axis=0), 2, axis=1)
        padded = jnp.pad(tall_rows, ((1, 1), (1, 1), (0, 0)))
        summed = jnp.zeros((4 * H * W, CU), jnp.float32)
        for tap_row in range(3):
            for tap_col in range(3):
                window = padded[tap_row:tap_row + 2 * H, tap_col:tap_col + 2 * W].reshape(-1, C)
                summed = summed + jnp.dot(window, upscale_weight[tap_row, tap_col], preferred_element_type=jnp.float32)
        return (summed + upscale_bias).astype(jnp.bfloat16).reshape(2 * H, 2 * W * CU)
    return lax.map(upscale_frame, expanded)
```

```python
import functools

import jax
import jax.numpy as jnp
from jax import lax
from jax.experimental import pallas as pl
from jax.experimental.pallas import tpu as pltpu
from jax.sharding import PartitionSpec as P

epsilon = 1e-06
bf16 = jnp.bfloat16
f32 = jnp.float32


def normed(values, scaling):
    return values * lax.rsqrt(jnp.mean(values * values, axis=-1, keepdims=True) + epsilon) * scaling


def silu(values):
    return values / (1.0 + jnp.exp(-values))


def dot(a, b):
    return jnp.dot(a, b, preferred_element_type=f32)


def fill_history(taps, row, act, frames):
    count, channels = act.shape
    columns = count // frames
    frame_of = lax.broadcasted_iota(jnp.int32, act.shape, 0) % frames
    for lag in (2, 1, 0):
        moved = act if lag == 0 else jnp.where(frame_of >= lag, pltpu.roll(act, lag, 0), 0.0)
        at = (2 - lag) * channels
        taps[row, :, :, at : at + channels] = moved.astype(bf16).reshape(columns, frames, channels)


def conv_step(taps, weight_ref, total, out_columns):
    step = pl.program_id(0)
    rows, _, frames, depth = taps.shape
    window = taps[pl.ds(step // 3, rows - 2), pl.ds(step % 3, out_columns)]
    part = dot(window.reshape(-1, depth), weight_ref[...].reshape(depth, -1))

    @pl.when(step == 0)
    def _():
        total[...] = part

    @pl.when(step > 0)
    def _():
        total[...] += part


def first_conv_kernel(
    chunk_ref, top, mid, bottom, gain, weight, bias, next_gain, out, taps, total, *, chunks
):
    rows, columns, frames, channels = mid.shape
    out_columns = columns - 2

    @pl.when(pl.program_id(0) == 0)
    def _():
        for row in range(rows + 2):
            source = top[0] if row == 0 else bottom[0] if row == rows + 1 else mid[row - 1]
            values = source.reshape(columns * frames, channels).astype(f32)
            fill_history(taps, row, silu(normed(values, gain[...])), frames)

    conv_step(taps, weight, total, out_columns)

    @pl.when(pl.program_id(0) == 8)
    def _():
        chunk = chunk_ref[0]
        shape = (out_columns * frames, channels)
        column = lax.broadcasted_iota(jnp.int32, shape, 0) // frames
        inside = ((column > 0) | (chunk > 0)) & ((column < out_columns - 1) | (chunk < chunks - 1))
        for row in range(rows):
            hidden = total[row * shape[0] : (row + 1) * shape[0]] + bias[...]
            act = silu(normed(hidden, next_gain[...]))
            out[row] = jnp.where(inside, act, 0.0).astype(bf16).reshape(out_columns, frames, channels)


def second_conv_kernel(top, mid, bottom, latent, weight, bias, out, taps, total):
    rows, columns, frames, channels = mid.shape
    out_columns = columns - 2

    @pl.when(pl.program_id(0) == 0)
    def _():
        for row in range(rows + 2):
            source = top[0] if row == 0 else bottom[0] if row == rows + 1 else mid[row - 1]
            values = source.reshape(columns * frames, channels).astype(f32)
            fill_history(taps, row, values, frames)

    conv_step(taps, weight, total, out_columns)

    @pl.when(pl.program_id(0) == 8)
    def _():
        size = out_columns * frames
        for row in range(rows):
            hidden = total[row * size : (row + 1) * size] + bias[...]
            own = latent[row, 2 : 2 + out_columns].reshape(size, channels).astype(f32)
            out[row] = (own + hidden).astype(bf16).reshape(out_columns, frames, channels)


def whole(array):
    return pl.BlockSpec(array.shape, lambda *_: (0,) * array.ndim)


def tap_spec(channels):
    return pl.BlockSpec((3, 1, 1, channels, channels), lambda s: (0, s // 3, s % 3, 0, 0))


def conv_call(kernel, ahead, weight, after, out_columns, scalar=None):
    mid = ahead[1]
    rows, columns, frames, channels = mid.shape
    scratch = [
        pltpu.VMEM((rows + 2, columns, frames, 3 * channels), bf16),
        pltpu.VMEM((rows * out_columns * frames, channels), f32),
    ]
    operands = (*ahead, weight, *after)
    in_specs = [whole(a) for a in ahead] + [tap_spec(channels)] + [whole(a) for a in after]
    if scalar is not None:
        operands = (scalar, *operands)
        in_specs = [pl.BlockSpec(memory_space=pltpu.SMEM)] + in_specs
    shape = (rows, out_columns, frames, channels)
    flops = 2 * 27 * rows * out_columns * frames * channels * channels
    return pl.pallas_call(
        kernel,
        grid=(9,),
        in_specs=in_specs,
        out_specs=pl.BlockSpec(shape, lambda s: (0, 0, 0, 0)),
        out_shape=jax.ShapeDtypeStruct(shape, bf16),
        scratch_shapes=scratch,
        compiler_params=pltpu.CompilerParams(dimension_semantics=("arbitrary",)),
        cost_estimate=pl.CostEstimate(
            flops=flops, transcendentals=0, bytes_accessed=2 * weight.size
        ),
    )(*operands)


def attend_kernel(*refs, first, last, blocks, chunk):
    refs = list(refs)
    take = lambda: refs.pop(0)
    keys_in = [take() for _ in range(blocks)]
    kv_weight, kv_bias = take(), take()
    if first:
        q_weight, q_bias = take(), take()
    else:
        q_in, peak_in, sum_in, held_in = take(), take(), take(), take()
    if last:
        source, out_weight, out_bias, out = take(), take(), take(), take()
    else:
        if first:
            q_out = take()
        peak_out, sum_out, held_out = take(), take(), take()
    channels = kv_weight.shape[0]
    scale = channels ** (-0.5)
    rows = jnp.concatenate([k[...] for k in keys_in], axis=0)
    pair = dot(rows, kv_weight[...]) + kv_bias[...]
    keys = pair[:, :channels].astype(bf16)
    values = pair[:, channels:].astype(bf16)
    count = keys_in[0].shape[0] if first else q_in.shape[0]
    for start in range(0, count, chunk):
        span = slice(start, start + chunk)
        if first:
            query = (dot(keys_in[0][span], q_weight[...]) + q_bias[...]).astype(bf16)
            q_out[span] = query
        else:
            query = q_in[span]
        scores = scale * lax.dot_general(
            query, keys, (((1,), (1,)), ((), ())), preferred_element_type=f32
        )
        top = jnp.max(scores, axis=-1, keepdims=True)
        if first:
            peak = top
        else:
            before = peak_in[span][:, :1]
            peak = jnp.maximum(before, top)
        exponent = jnp.exp(scores - peak)
        summed = jnp.sum(exponent, axis=-1, keepdims=True)
        held = dot(exponent.astype(bf16), values)
        if not first:
            fade = jnp.exp(before - peak)
            summed = summed + fade * sum_in[span][:, :1]
            held = held + fade * held_in[span]
        if last:
            attended = (held / summed).astype(bf16)
            mixed = source[span].astype(f32) + dot(attended, out_weight[...]) + out_bias[...]
            out[span] = mixed.astype(bf16)
        else:
            peak_out[span] = jnp.broadcast_to(peak, (chunk, 128))
            sum_out[span] = jnp.broadcast_to(summed, (chunk, 128))
            held_out[span] = held


def attend_call(key_blocks, kv_weight, kv_bias, extra, first, last):
    channels = kv_weight.shape[0]
    count = extra[0].shape[0] if not first else key_blocks[0].shape[0]
    total_keys = sum(k.shape[0] for k in key_blocks)
    state = [
        jax.ShapeDtypeStruct((count, 128), f32),
        jax.ShapeDtypeStruct((count, 128), f32),
        jax.ShapeDtypeStruct((count, channels), f32),
    ]
    if last:
        out_shape = jax.ShapeDtypeStruct((count, channels), bf16)
    elif first:
        out_shape = [jax.ShapeDtypeStruct((count, channels), bf16)] + state
    else:
        out_shape = state
    flops = 4 * total_keys * channels * (channels + count)
    return pl.pallas_call(
        functools.partial(
            attend_kernel, first=first, last=last, blocks=len(key_blocks), chunk=128
        ),
        out_shape=out_shape,
        cost_estimate=pl.CostEstimate(
            flops=flops, transcendentals=count * total_keys, bytes_accessed=4 * count * channels
        ),
    )(*key_blocks, kv_weight, kv_bias, *extra)


def attention(blocked, gain, project_weight, project_bias, output_weight, output_bias):
    count, channels = blocked.shape
    own = normed(blocked.astype(f32), gain).astype(bf16)
    rows = lax.axis_size("row")
    swap = [(i, i ^ 1) for i in range(rows)]
    onward = [(i, (i + (2 if i % 2 == 0 else -2)) % rows) for i in range(rows)]
    partner = lax.ppermute(own, "row", swap)
    near = lax.ppermute(jnp.concatenate([own, partner], 0), "row", onward)
    far = lax.ppermute(near[:count], "row", onward)
    near_too = lax.ppermute(near, "row", swap)
    far_too = lax.ppermute(far, "row", swap)
    kv_weight = project_weight[:, channels:]
    kv_bias = project_bias[channels:].reshape(1, -1)
    q_weight = project_weight[:, :channels]
    q_bias = project_bias[:channels].reshape(1, -1)
    query, *state = attend_call([own, partner], kv_weight, kv_bias, (q_weight, q_bias), True, False)
    state = attend_call([near], kv_weight, kv_bias, (query, *state), False, False)
    state = attend_call([near_too], kv_weight, kv_bias, (query, *state), False, False)
    extra = (query, *state, blocked, output_weight, output_bias.reshape(1, -1))
    return attend_call([far, far_too], kv_weight, kv_bias, extra, False, True)


def merged_taps(weight):
    depth = weight.shape[2]
    wide = weight.astype(f32)
    by_row = [(wide[0], wide[1] + wide[2]), (wide[0] + wide[1], wide[2])]
    fill = 256 - weight.shape[3]
    result = []
    for pair in by_row:
        for parity in range(2):
            pads = (0, fill) if parity == 0 else (fill, 0)
            taps = []
            for row in pair:
                columns = (row[0], row[1] + row[2]) if parity == 0 else (row[0] + row[1], row[2])
                taps += [jnp.pad(c, ((0, 0), pads)) for c in columns]
            result.append(jnp.concatenate(taps, axis=0).astype(bf16))
    return jnp.stack(result).reshape(2, 2, 4 * depth, 256)


def upscale_kernel(top, mid, bottom, weight, bias, out, taps, total):
    rows, columns, channels = mid.shape
    at = lax.broadcasted_iota(jnp.int32, (columns, channels), 0)
    for row in range(rows + 2):
        source = top[0] if row == 0 else bottom[0] if row == rows + 1 else mid[row - 1]
        values = source.astype(f32)
        before = jnp.where(at > 0, pltpu.roll(values, 1, 0), 0.0)
        after = jnp.where(at < columns - 1, pltpu.roll(values, columns - 1, 0), 0.0)
        taps[row, :, :channels] = before.astype(bf16)
        taps[row, :, channels : 2 * channels] = source
        taps[row, :, 2 * channels :] = after.astype(bf16)
    for parity in range(2):
        parts = []
        for side in range(2):
            lanes = slice(side * channels, side * channels + 2 * channels)
            upper = taps[parity : parity + rows, :, lanes].reshape(rows * columns, 2 * channels)
            lower = taps[parity + 1 : parity + 1 + rows, :, lanes].reshape(
                rows * columns, 2 * channels
            )
            parts.append(
                dot(upper, weight[parity, side, : 2 * channels])
                + dot(lower, weight[parity, side, 2 * channels :])
            )
        left, right = parts
        joined = [left[:, :128], left[:, 128:] + right[:, :128], right[:, 128:]]
        for row in range(rows):
            span = slice(row * columns, (row + 1) * columns)
            start = (2 * row + parity) * columns
            for third in range(3):
                lanes = slice(third * 128, (third + 1) * 128)
                total[third, start : start + columns, :] = joined[third][span] + bias[:, lanes]

    def emit(column, carry):
        for third in range(3):
            rows_here = total[third, pl.ds(column, 2 * rows, stride=columns), :]
            start = pl.multiple_of(column * channels + third * 128, 128)
            out[0, :, pl.ds(start, 128)] = rows_here.astype(bf16)
        return carry

    lax.fori_loop(0, columns, emit, 0, unroll=4)


def upscale(top, mid, bottom, weight, bias):
    rows, columns, channels = mid.shape[0], mid.shape[1], mid.shape[2] // 2
    width = weight.shape[-1]
    assert 2 * width == channels and channels == 384
    taps = merged_taps(weight)
    wide_bias = jnp.concatenate([bias, bias]).reshape(1, -1)
    return pl.pallas_call(
        upscale_kernel,
        grid=(2,),
        in_specs=[
            pl.BlockSpec((1, columns, channels), lambda h: (0, 0, h)),
            pl.BlockSpec((rows, columns, channels), lambda h: (0, 0, h)),
            pl.BlockSpec((1, columns, channels), lambda h: (0, 0, h)),
            whole(taps),
            whole(wide_bias),
        ],
        out_specs=pl.BlockSpec((1, 2 * rows, columns * channels), lambda h: (h, 0, 0)),
        out_shape=jax.ShapeDtypeStruct((2, 2 * rows, columns * channels), bf16),
        scratch_shapes=[
            pltpu.VMEM((rows + 2, columns, 3 * channels), bf16),
            pltpu.VMEM((3, 2 * rows * columns, 128), f32),
        ],
        compiler_params=pltpu.CompilerParams(dimension_semantics=("arbitrary",)),
        cost_estimate=pl.CostEstimate(
            flops=2 * 2 * rows * columns * 16 * channels * width,
            transcendentals=0,
            bytes_accessed=8 * rows * columns * channels,
        ),
    )(top, mid, bottom, taps, wide_bias)


def exchange(pieces):
    return lax.all_to_all(pieces, "frame", 0, 0)


def row_rims(values):
    rows = lax.axis_size("row")
    top = lax.ppermute(values[-1:], "row", [(i, i + 1) for i in range(rows - 1)])
    bottom = lax.ppermute(values[:1], "row", [(i + 1, i) for i in range(rows - 1)])
    return top, bottom


def on_device(
    latent,
    first_gain,
    first_weight,
    first_bias,
    second_gain,
    second_weight,
    second_bias,
    attend_gain,
    project_weight,
    project_bias,
    output_weight,
    output_bias,
    temporal_weight,
    temporal_bias,
    upscale_weight,
    upscale_bias,
):
    _, rows, columns, channels = latent.shape
    chunks = lax.axis_size("frame")
    width = columns // chunks
    line = lambda v: v.reshape(1, -1)
    chunk = lax.axis_index("frame").astype(jnp.int32).reshape(1)

    wide = jnp.pad(latent[0], ((0, 0), (2, 2), (0, 0)))
    windows = jnp.stack([wide[:, k * width : (k + 1) * width + 4] for k in range(chunks)])
    source = exchange(windows).transpose(1, 2, 0, 3)
    top, bottom = row_rims(source)
    second_act = conv_call(
        functools.partial(first_conv_kernel, chunks=chunks),
        (top, source, bottom, line(first_gain)),
        first_weight,
        (line(first_bias), line(second_gain)),
        width + 2,
        chunk,
    )
    top, bottom = row_rims(second_act)
    blocked = conv_call(
        second_conv_kernel,
        (top, second_act, bottom, source),
        second_weight,
        (line(second_bias),),
        width,
    )
    blocked = blocked.reshape(rows * width, chunks, channels).transpose(1, 0, 2)
    blocked = exchange(blocked).reshape(-1, channels)
    mixed = attention(
        blocked, attend_gain, project_weight, project_bias, output_weight, output_bias
    )
    mixed = exchange(mixed.reshape(chunks, rows * width, channels))
    padded = jnp.pad(mixed, ((2, 0), (0, 0), (0, 0)))
    stacked = jnp.concatenate([padded[t : t + chunks] for t in range(3)], axis=-1)
    doubled = dot(
        stacked.reshape(-1, 3 * channels), temporal_weight.reshape(3 * channels, -1)
    )
    doubled = (doubled + temporal_bias).astype(bf16)
    doubled = exchange(doubled.reshape(chunks, rows * width, 2 * channels))
    doubled = doubled.reshape(chunks, rows, width, 2 * channels)
    doubled = doubled.transpose(1, 0, 2, 3).reshape(rows, columns, 2 * channels)
    top, bottom = row_rims(doubled)
    return upscale(top, doubled, bottom, upscale_weight, upscale_bias)


def solution(mesh):
    placed = (P("frame", "row", None, None),) + (P(),) * 15
    return jax.shard_map(
        on_device, mesh=mesh, in_specs=placed, out_specs=P("frame", "row", None), check_vma=False
    )
```

```python
import functools

import jax
import jax.numpy as jnp
from jax import lax
from jax.experimental import pallas as pl
from jax.experimental.pallas import tpu as pltpu
from jax.sharding import PartitionSpec as P

epsilon = 1e-06
bf16 = jnp.bfloat16
f32 = jnp.float32


def normed(values, scaling):
    return values * lax.rsqrt(jnp.mean(values * values, axis=-1, keepdims=True) + epsilon) * scaling


def silu(values):
    return values / (1.0 + jnp.exp(-values))


def dot(a, b):
    return jnp.dot(a, b, preferred_element_type=f32)


def fill_history(taps, row, act, frames):
    count, channels = act.shape
    columns = count // frames
    frame_of = lax.broadcasted_iota(jnp.int32, act.shape, 0) & (frames - 1)
    for lag in (2, 1, 0):
        moved = act if lag == 0 else jnp.where(frame_of >= lag, pltpu.roll(act, lag, 0), 0.0)
        at = (2 - lag) * channels
        taps[row, :, :, at : at + channels] = moved.astype(bf16).reshape(columns, frames, channels)


def conv_step(taps, weight_ref, total, out_columns):
    step = pl.program_id(0)
    rows, _, frames, depth = taps.shape
    part = 0.0
    for tap in range(3):
        window = taps[pl.ds(step, rows - 2), tap : tap + out_columns]
        weight = weight_ref[:, 0, tap].reshape(depth, -1)
        part = part + dot(window.reshape(-1, depth), weight)

    @pl.when(step == 0)
    def _():
        total[...] = part

    @pl.when(step > 0)
    def _():
        total[...] += part


def first_conv_kernel(
    chunk_ref, top, mid, bottom, lines, weight, out, taps, total, *, chunks
):
    rows, columns, frames, channels = mid.shape
    out_columns = columns - 2

    @pl.when(pl.program_id(0) == 0)
    def _():
        for row in range(rows + 2):
            source = top[0] if row == 0 else bottom[0] if row == rows + 1 else mid[row - 1]
            values = source.reshape(columns * frames, channels).astype(f32)
            fill_history(taps, row, silu(normed(values, lines[0:1])), frames)

    conv_step(taps, weight, total, out_columns)

    @pl.when(pl.program_id(0) == 2)
    def _():
        chunk = chunk_ref[0]
        shape = (out_columns * frames, channels)
        column = lax.broadcasted_iota(jnp.int32, shape, 0) // frames
        inside = ((column > 0) | (chunk > 0)) & ((column < out_columns - 1) | (chunk < chunks - 1))
        for row in range(rows):
            hidden = total[row * shape[0] : (row + 1) * shape[0]] + lines[1:2]
            act = silu(normed(hidden, lines[2:3]))
            out[row] = jnp.where(inside, act, 0.0).astype(bf16).reshape(out_columns, frames, channels)


def second_conv_kernel(top, mid, bottom, latent, lines, weight, out, taps, total):
    rows, columns, frames, channels = mid.shape
    out_columns = columns - 2

    @pl.when(pl.program_id(0) == 0)
    def _():
        for row in range(rows + 2):
            source = top[0] if row == 0 else bottom[0] if row == rows + 1 else mid[row - 1]
            values = source.reshape(columns * frames, channels).astype(f32)
            fill_history(taps, row, values, frames)

    conv_step(taps, weight, total, out_columns)

    @pl.when(pl.program_id(0) == 2)
    def _():
        size = out_columns * frames
        for row in range(rows):
            hidden = total[row * size : (row + 1) * size] + lines[3:4]
            own = latent[row, 2 : 2 + out_columns].reshape(size, channels).astype(f32)
            out[row] = (own + hidden).astype(bf16).reshape(out_columns, frames, channels)


def whole(array):
    return pl.BlockSpec(array.shape, lambda *_: (0,) * array.ndim)


def tap_spec(channels):
    return pl.BlockSpec((3, 1, 3, channels, channels), lambda s: (0, s, 0, 0, 0))


def conv_call(kernel, ahead, weight, out_columns, scalar=None):
    mid = ahead[1]
    rows, columns, frames, channels = mid.shape
    scratch = [
        pltpu.VMEM((rows + 2, columns, frames, 3 * channels), bf16),
        pltpu.VMEM((rows * out_columns * frames, channels), f32),
    ]
    operands = (*ahead, weight)
    in_specs = [whole(a) for a in ahead] + [tap_spec(channels)]
    if scalar is not None:
        operands = (scalar, *operands)
        in_specs = [pl.BlockSpec(memory_space=pltpu.SMEM)] + in_specs
    shape = (rows, out_columns, frames, channels)
    flops = 2 * 27 * rows * out_columns * frames * channels * channels
    return pl.pallas_call(
        kernel,
        grid=(3,),
        in_specs=in_specs,
        out_specs=pl.BlockSpec(shape, lambda s: (0, 0, 0, 0)),
        out_shape=jax.ShapeDtypeStruct(shape, bf16),
        scratch_shapes=scratch,
        compiler_params=pltpu.CompilerParams(dimension_semantics=("arbitrary",)),
        cost_estimate=pl.CostEstimate(
            flops=flops, transcendentals=0, bytes_accessed=2 * weight.size
        ),
    )(*operands)


def attend_kernel(*refs, first, last, blocks, span):
    refs = list(refs)
    take = lambda: refs.pop(0)
    keys_in = [take() for _ in range(blocks)]
    lines, key_weight, value_weight = take(), take(), take()
    if first:
        q_weight = take()
    else:
        q_in, peak_in, sum_in, held_in = take(), take(), take(), take()
    if last:
        source, out_weight, out = take(), take(), take()
    else:
        if first:
            q_out = take()
        peak_out, sum_out, held_out = take(), take(), take()
    channels = key_weight.shape[0]
    factor = channels ** (-0.5) * 1.4426950408889634
    rows = jnp.concatenate([k[...] for k in keys_in], axis=0)
    keys = (dot(rows, key_weight[...]) + lines[6:7]).astype(bf16)
    values = (across(value_weight[...], rows) + upright(lines[7:8])).astype(bf16)
    count = keys_in[0].shape[0] if first else q_in.shape[1]
    for start in range(0, count, span):
        at = slice(start, min(count, start + span))
        if first:
            query = (across(q_weight[...], keys_in[0][at]) + upright(lines[5:6])).astype(bf16)
            q_out[:, at] = query
        else:
            query = q_in[:, at]
        scores = dot(keys, query)
        peak = jnp.max(scores, axis=0, keepdims=True)
        if not first:
            before = peak_in[:, at]
            peak = jnp.maximum(before, peak)
        exponent = jnp.exp2((scores - peak) * factor)
        summed = jnp.sum(exponent, axis=0, keepdims=True)
        held = dot(values, exponent.astype(bf16))
        if not first:
            fade = jnp.exp2((before - peak) * factor)
            summed = summed + fade * sum_in[:, at]
            held = held + fade * held_in[:, at]
        if last:
            attended = (held / summed).astype(bf16)
            mixed = lax.dot_general(
                attended, out_weight[...], (((0,), (0,)), ((), ())), preferred_element_type=f32
            )
            out[at] = (source[at].astype(f32) + mixed + lines[8:9]).astype(bf16)
        else:
            peak_out[:, at] = peak
            sum_out[:, at] = summed
            held_out[:, at] = held


def upright(line):
    return jnp.broadcast_to(line, (128, line.shape[1])).T[:, :1]


def across(a, b):
    return lax.dot_general(a, b, (((1,), (1,)), ((), ())), preferred_element_type=f32)


def attend_call(key_blocks, weights, extra, first, last):
    channels = weights[1].shape[0]
    count = key_blocks[0].shape[0] if first else extra[0].shape[1]
    total_keys = sum(k.shape[0] for k in key_blocks)
    state = [
        jax.ShapeDtypeStruct((1, count), f32),
        jax.ShapeDtypeStruct((1, count), f32),
        jax.ShapeDtypeStruct((channels, count), f32),
    ]
    if last:
        out_shape = jax.ShapeDtypeStruct((count, channels), bf16)
    elif first:
        out_shape = [jax.ShapeDtypeStruct((channels, count), bf16)] + state
    else:
        out_shape = state
    flops = 4 * total_keys * channels * (channels + count)
    return pl.pallas_call(
        functools.partial(
            attend_kernel, first=first, last=last, blocks=len(key_blocks), span=256
        ),
        out_shape=out_shape,
        cost_estimate=pl.CostEstimate(
            flops=2 * flops, transcendentals=count * total_keys, bytes_accessed=4 * count * channels
        ),
    )(*key_blocks, *weights, *extra)


def settle_kernel(pieces, lines, blocked, normal, gathered, placed):
    chunks, size, channels = pieces.shape
    rows = placed.shape[0]
    width = size // rows
    gathered[...] = pieces[...].reshape(chunks * size, channels).astype(f32)
    for chunk in range(chunks):
        for row in range(rows):
            at = chunk * size + row * width
            placed[row, chunk * width : (chunk + 1) * width] = gathered[at : at + width]
    for row in range(rows):
        columns = chunks * width
        span = slice(row * columns, (row + 1) * columns)
        values = placed[row].astype(bf16)
        blocked[span] = values
        normal[span] = normed(values.astype(f32), lines[4:5]).astype(bf16)


def settle(pieces, lines, rows):
    chunks, size, channels = pieces.shape
    count = chunks * size
    return pl.pallas_call(
        settle_kernel,
        out_shape=[jax.ShapeDtypeStruct((count, channels), bf16)] * 2,
        scratch_shapes=[
            pltpu.VMEM((count, channels), f32),
            pltpu.VMEM((rows, count // rows, channels), f32),
        ],
        cost_estimate=pl.CostEstimate(
            flops=10 * count * channels, transcendentals=0, bytes_accessed=6 * count * channels
        ),
    )(pieces, lines)


def attention(blocked, own, weights, q_weight, output_weight):
    rows = lax.axis_size("row")
    swap = [(i, i ^ 1) for i in range(rows)]
    onward = [(i, (i + (2 if i % 2 == 0 else -2)) % rows) for i in range(rows)]
    send = lambda block, route: lax.ppermute(block, "row", route)
    near_a = send(own, onward)
    partner = send(own, swap)
    near_b = send(partner, onward)
    query, *state = attend_call([own, partner], weights, (q_weight,), True, False)
    near_a, near_b, query = lax.optimization_barrier((near_a, near_b, query))
    far = send(near_a, onward)
    near = [near_a, near_b, send(near_a, swap), send(near_b, swap)]
    state = attend_call(near, weights, (query, *state), False, False)
    far, state = lax.optimization_barrier((far, state))
    far_too = send(far, swap)
    extra = (query, *state, blocked, output_weight)
    return attend_call([far, far_too], weights, extra, False, True)


def merge_kernel(weight, out):
    row = [[weight[i, j].astype(f32) for j in range(3)] for i in range(3)]
    depth = weight.shape[2]
    for parity in range(2):
        if parity == 0:
            upper, lower = row[0], [a + b for a, b in zip(row[1], row[2])]
        else:
            upper, lower = [a + b for a, b in zip(row[0], row[1])], row[2]
        for tap, line in enumerate((upper, lower)):
            for side in range(2):
                pair = (line[0], line[1] + line[2]) if side == 0 else (line[0] + line[1], line[2])
                for place, value in enumerate(pair):
                    if side == 1:
                        value = pltpu.roll(value, 64, 1)
                    at = (2 * tap + place) * depth
                    out[parity, side, at : at + depth] = value.astype(bf16)


def merged_taps(weight):
    depth = weight.shape[2]
    padded = jnp.pad(weight, ((0, 0), (0, 0), (0, 0), (0, 256 - weight.shape[3])))
    return pl.pallas_call(
        merge_kernel,
        out_shape=jax.ShapeDtypeStruct((2, 2, 4 * depth, 256), bf16),
        cost_estimate=pl.CostEstimate(
            flops=2 * 10**9, transcendentals=0, bytes_accessed=6 * 10**6
        ),
    )(padded)


def upscale_kernel(top, mid, bottom, weight, bias, out, taps, total):
    rows, columns, channels = mid.shape
    at = lax.broadcasted_iota(jnp.int32, (columns, channels), 0)
    for row in range(rows + 2):
        source = top[0] if row == 0 else bottom[0] if row == rows + 1 else mid[row - 1]
        values = source.astype(f32)
        before = jnp.where(at > 0, pltpu.roll(values, 1, 0), 0.0)
        after = jnp.where(at < columns - 1, pltpu.roll(values, columns - 1, 0), 0.0)
        taps[row, :, :channels] = before.astype(bf16)
        taps[row, :, channels : 2 * channels] = source
        taps[row, :, 2 * channels :] = after.astype(bf16)
    for parity in range(2):
        parts = []
        for side in range(2):
            lanes = slice(side * channels, side * channels + 2 * channels)
            upper = taps[parity : parity + rows, :, lanes].reshape(rows * columns, 2 * channels)
            lower = taps[parity + 1 : parity + 1 + rows, :, lanes].reshape(
                rows * columns, 2 * channels
            )
            parts.append(
                dot(upper, weight[parity, side, : 2 * channels])
                + dot(lower, weight[parity, side, 2 * channels :])
            )
        left, right = parts
        joined = [left[:, :128], left[:, 128:] + right[:, :128], right[:, 128:]]
        for row in range(rows):
            span = slice(row * columns, (row + 1) * columns)
            start = (2 * row + parity) * columns
            for third in range(3):
                lanes = slice(third * 128, (third + 1) * 128)
                total[third, start : start + columns, :] = joined[third][span] + bias[9:10, lanes]

    def emit(column, carry):
        for third in range(3):
            rows_here = total[third, pl.ds(column, 2 * rows, stride=columns), :]
            start = pl.multiple_of(column * channels + third * 128, 128)
            out[0, :, pl.ds(start, 128)] = rows_here.astype(bf16)
        return carry

    lax.fori_loop(0, columns, emit, 0, unroll=4)


def upscale(top, mid, bottom, taps, lines):
    rows, columns, channels = mid.shape[0], mid.shape[1], mid.shape[2] // 2
    width = channels // 2
    return pl.pallas_call(
        upscale_kernel,
        grid=(2,),
        in_specs=[
            pl.BlockSpec((1, columns, channels), lambda h: (0, 0, h)),
            pl.BlockSpec((rows, columns, channels), lambda h: (0, 0, h)),
            pl.BlockSpec((1, columns, channels), lambda h: (0, 0, h)),
            whole(taps),
            whole(lines),
        ],
        out_specs=pl.BlockSpec((1, 2 * rows, columns * channels), lambda h: (h, 0, 0)),
        out_shape=jax.ShapeDtypeStruct((2, 2 * rows, columns * channels), bf16),
        scratch_shapes=[
            pltpu.VMEM((rows + 2, columns, 3 * channels), bf16),
            pltpu.VMEM((3, 2 * rows * columns, 128), f32),
        ],
        compiler_params=pltpu.CompilerParams(dimension_semantics=("arbitrary",)),
        cost_estimate=pl.CostEstimate(
            flops=2 * 2 * rows * columns * 16 * channels * width,
            transcendentals=0,
            bytes_accessed=8 * rows * columns * channels,
        ),
    )(top, mid, bottom, taps, lines)


def exchange(pieces):
    return lax.all_to_all(pieces, "frame", 0, 0)


def row_rims(last, first):
    rows = lax.axis_size("row")
    top = lax.ppermute(last, "row", [(i, i + 1) for i in range(rows - 1)])
    bottom = lax.ppermute(first, "row", [(i + 1, i) for i in range(rows - 1)])
    return top, bottom


def pack_kernel(latent, out, wide):
    chunks, rows, size, channels = out.shape
    columns = latent.shape[1]
    zeros = jnp.zeros((8, channels), f32)
    for row in range(rows):
        wide[row, 0:8] = zeros
        wide[row, 8 : 8 + columns] = latent[row].astype(f32)
        wide[row, 8 + columns :] = zeros
        for chunk in range(chunks):
            at = 6 + chunk * (size - 4)
            out[chunk, row] = wide[row, at : at + size].astype(bf16)


def pack(latent, chunks):
    rows, columns, channels = latent.shape
    size = columns // chunks + 4
    return pl.pallas_call(
        pack_kernel,
        out_shape=jax.ShapeDtypeStruct((chunks, rows, size, channels), bf16),
        scratch_shapes=[pltpu.VMEM((rows, columns + 16, channels), f32)],
        cost_estimate=pl.CostEstimate(
            flops=latent.size, transcendentals=0, bytes_accessed=5 * latent.size
        ),
    )(latent)


def on_device(
    latent,
    first_gain,
    first_weight,
    first_bias,
    second_gain,
    second_weight,
    second_bias,
    attend_gain,
    project_weight,
    project_bias,
    output_weight,
    output_bias,
    temporal_weight,
    temporal_bias,
    upscale_weight,
    upscale_bias,
):
    _, rows, columns, channels = latent.shape
    chunks = lax.axis_size("frame")
    width = columns // chunks
    chunk = lax.axis_index("frame").astype(jnp.int32).reshape(1)

    turned = project_weight.T
    lines = [first_gain, first_bias, second_gain, second_bias, attend_gain]
    lines += [project_bias[k * channels : (k + 1) * channels] for k in range(3)]
    lines += [output_bias, jnp.concatenate([upscale_bias, upscale_bias])]
    prepared = (
        jnp.stack(lines),
        project_weight[:, channels : 2 * channels],
        turned[2 * channels :],
        turned[:channels],
        merged_taps(upscale_weight),
    )
    source = exchange(pack(latent[0], chunks)).transpose(1, 2, 0, 3)
    last, prepared = lax.optimization_barrier((source[-1:], prepared))
    lines, key_weight, value_weight, q_weight, taps = prepared
    top, bottom = row_rims(last, source[:1])
    second_act = conv_call(
        functools.partial(first_conv_kernel, chunks=chunks),
        (top, source, bottom, lines),
        first_weight,
        width + 2,
        chunk,
    )
    top, bottom = row_rims(second_act[-1:], second_act[:1])
    blocked = conv_call(
        second_conv_kernel, (top, second_act, bottom, source, lines), second_weight, width
    )
    blocked = blocked.reshape(rows * width, chunks, channels).transpose(1, 0, 2)
    blocked, own = settle(exchange(blocked), lines, rows)
    mixed = attention(blocked, own, (lines, key_weight, value_weight), q_weight, output_weight)
    earlier = [
        lax.ppermute(mixed, "frame", [(i, i + lag) for i in range(chunks - lag)]) for lag in (2, 1)
    ]
    stacked = jnp.concatenate([*earlier, mixed], axis=-1)
    doubled = dot(stacked, temporal_weight.reshape(3 * channels, -1))
    doubled = (doubled + temporal_bias).astype(bf16).reshape(rows, columns, 2 * channels)
    top, bottom = row_rims(doubled[-1:], doubled[:1])
    return upscale(top, doubled, bottom, taps, lines)


def solution(mesh):
    placed = (P("frame", "row", None, None),) + (P(),) * 15
    return jax.shard_map(
        on_device, mesh=mesh, in_specs=placed, out_specs=P("frame", "row", None), check_vma=False
    )
```

```python
import functools

import jax
import jax.numpy as jnp
from jax import lax
from jax.experimental import pallas as pl
from jax.experimental.pallas import tpu as pltpu
from jax.sharding import PartitionSpec as P

epsilon = 1e-06
bf16 = jnp.bfloat16
f32 = jnp.float32


def normed(values, scaling):
    return values * lax.rsqrt(jnp.mean(values * values, axis=-1, keepdims=True) + epsilon) * scaling


def silu(values):
    return values / (1.0 + jnp.exp(-values))


def dot(a, b):
    return jnp.dot(a, b, preferred_element_type=f32)


def fill_history(taps, row, act, frames):
    count, channels = act.shape
    columns = count // frames
    frame_of = lax.broadcasted_iota(jnp.int32, act.shape, 0) & (frames - 1)
    for lag in (2, 1, 0):
        moved = act if lag == 0 else jnp.where(frame_of >= lag, pltpu.roll(act, lag, 0), 0.0)
        at = (2 - lag) * channels
        taps[row, :, :, at : at + channels] = moved.astype(bf16).reshape(columns, frames, channels)


def conv_step(taps, weight_ref, total, out_columns):
    step = pl.program_id(0)
    rows, _, frames, depth = taps.shape
    part = 0.0
    for tap in range(3):
        window = taps[pl.ds(step, rows - 2), tap : tap + out_columns]
        weight = weight_ref[:, 0, tap].reshape(depth, -1)
        part = part + dot(window.reshape(-1, depth), weight)

    @pl.when(step == 0)
    def _():
        total[...] = part

    @pl.when(step > 0)
    def _():
        total[...] += part


def first_conv_kernel(
    chunk_ref, top, mid, bottom, lines, weight, out, taps, total, *, chunks
):
    rows, columns, frames, channels = mid.shape
    out_columns = columns - 2

    @pl.when(pl.program_id(0) == 0)
    def _():
        for row in range(rows + 2):
            source = top[0] if row == 0 else bottom[0] if row == rows + 1 else mid[row - 1]
            values = source.reshape(columns * frames, channels).astype(f32)
            fill_history(taps, row, silu(normed(values, lines[0:1])), frames)

    conv_step(taps, weight, total, out_columns)

    @pl.when(pl.program_id(0) == 2)
    def _():
        chunk = chunk_ref[0]
        shape = (out_columns * frames, channels)
        column = lax.broadcasted_iota(jnp.int32, shape, 0) // frames
        inside = ((column > 0) | (chunk > 0)) & ((column < out_columns - 1) | (chunk < chunks - 1))
        for row in range(rows):
            hidden = total[row * shape[0] : (row + 1) * shape[0]] + lines[1:2]
            act = silu(normed(hidden, lines[2:3]))
            out[row] = jnp.where(inside, act, 0.0).astype(bf16).reshape(out_columns, frames, channels)


def second_conv_kernel(top, mid, bottom, latent, lines, weight, out, taps, total):
    rows, columns, frames, channels = mid.shape
    out_columns = columns - 2

    @pl.when(pl.program_id(0) == 0)
    def _():
        for row in range(rows + 2):
            source = top[0] if row == 0 else bottom[0] if row == rows + 1 else mid[row - 1]
            values = source.reshape(columns * frames, channels).astype(f32)
            fill_history(taps, row, values, frames)

    conv_step(taps, weight, total, out_columns)

    @pl.when(pl.program_id(0) == 2)
    def _():
        size = out_columns * frames
        for row in range(rows):
            hidden = total[row * size : (row + 1) * size] + lines[3:4]
            own = latent[row, 2 : 2 + out_columns].reshape(size, channels).astype(f32)
            out[row] = (own + hidden).astype(bf16).reshape(out_columns, frames, channels)


def whole(array):
    return pl.BlockSpec(array.shape, lambda *_: (0,) * array.ndim)


def tap_spec(channels):
    return pl.BlockSpec((3, 1, 3, channels, channels), lambda s: (0, s, 0, 0, 0))


def conv_call(kernel, ahead, weight, out_columns, scalar=None):
    mid = ahead[1]
    rows, columns, frames, channels = mid.shape
    scratch = [
        pltpu.VMEM((rows + 2, columns, frames, 3 * channels), bf16),
        pltpu.VMEM((rows * out_columns * frames, channels), f32),
    ]
    operands = (*ahead, weight)
    in_specs = [whole(a) for a in ahead] + [tap_spec(channels)]
    if scalar is not None:
        operands = (scalar, *operands)
        in_specs = [pl.BlockSpec(memory_space=pltpu.SMEM)] + in_specs
    shape = (rows, out_columns, frames, channels)
    flops = 2 * 27 * rows * out_columns * frames * channels * channels
    return pl.pallas_call(
        kernel,
        grid=(3,),
        in_specs=in_specs,
        out_specs=pl.BlockSpec(shape, lambda s: (0, 0, 0, 0)),
        out_shape=jax.ShapeDtypeStruct(shape, bf16),
        scratch_shapes=scratch,
        compiler_params=pltpu.CompilerParams(dimension_semantics=("arbitrary",)),
        cost_estimate=pl.CostEstimate(
            flops=flops, transcendentals=0, bytes_accessed=2 * weight.size
        ),
    )(*operands)


def attend_kernel(*refs, first, last, blocks, span):
    refs = list(refs)
    take = lambda: refs.pop(0)
    keys_in = [take() for _ in range(blocks)]
    lines, key_weight, value_weight = take(), take(), take()
    if first:
        q_weight = take()
    else:
        q_in, peak_in, sum_in, held_in = take(), take(), take(), take()
    if last:
        source, out_weight, *outs = take(), take(), take(), take()
    else:
        if first:
            q_out = take()
        peak_out, sum_out, held_out = take(), take(), take()
    channels = key_weight.shape[0]
    factor = channels ** (-0.5) * 1.4426950408889634
    rows = jnp.concatenate([k[...] for k in keys_in], axis=0)
    keys = (dot(rows, key_weight[...]) + lines[6:7]).astype(bf16)
    values = (across(value_weight[...], rows) + upright(lines[7:8])).astype(bf16)
    count = keys_in[0].shape[0] if first else q_in.shape[1]
    for start in range(0, count, span):
        at = slice(start, min(count, start + span))
        if first:
            query = (across(q_weight[...], keys_in[0][at]) + upright(lines[5:6])).astype(bf16)
            q_out[:, at] = query
        else:
            query = q_in[:, at]
        scores = dot(keys, query)
        peak = jnp.max(scores, axis=0, keepdims=True)
        if not first:
            before = peak_in[:, at]
            peak = jnp.maximum(before, peak)
        exponent = jnp.exp2((scores - peak) * factor)
        summed = jnp.sum(exponent, axis=0, keepdims=True)
        held = dot(values, exponent.astype(bf16))
        if not first:
            fade = jnp.exp2((before - peak) * factor)
            summed = summed + fade * sum_in[:, at]
            held = held + fade * held_in[:, at]
        if last:
            attended = (held / summed).astype(bf16)
            mixed = lax.dot_general(
                attended, out_weight[...], (((0,), (0,)), ((), ())), preferred_element_type=f32
            )
            mixed = (source[at].astype(f32) + mixed + lines[8:9]).astype(bf16)
            half = outs[0].shape[0]
            for part, out in enumerate(outs):
                low, high = max(at.start, part * half), min(at.stop, (part + 1) * half)
                if low < high:
                    shift = part * half
                    out[low - shift : high - shift] = mixed[low - at.start : high - at.start]
        else:
            peak_out[:, at] = peak
            sum_out[:, at] = summed
            held_out[:, at] = held


def upright(line):
    return jnp.broadcast_to(line, (128, line.shape[1])).T[:, :1]


def across(a, b):
    return lax.dot_general(a, b, (((1,), (1,)), ((), ())), preferred_element_type=f32)


def attend_middle_kernel(
    *refs, blocks, span
):
    sources, refs = refs[:blocks], refs[blocks:]
    lines, key_weight, value_weight, q_in, peak_in, sum_in, held_in = refs[:7]
    peak_out, sum_out, held_out, arrived, done = refs[7:]
    channels = key_weight.shape[0]
    factor = channels ** (-0.5) * 1.4426950408889634
    for index, source in enumerate(sources):
        pltpu.make_async_copy(source, arrived.at[index], done.at[index]).start()
    peak_out[...] = peak_in[...]
    sum_out[...] = sum_in[...]
    held_out[...] = held_in[...]
    key_bias = lines[6:7]
    value_bias = upright(lines[7:8])

    def step(index, carry):
        for half in range(2):
            slot = 2 * index + half
            pltpu.make_async_copy(sources[0], arrived.at[slot], done.at[slot]).wait()
        rows = arrived[pl.ds(2 * index, 2)].reshape(-1, channels)
        keys = (dot(rows, key_weight[...]) + key_bias).astype(bf16)
        values = (across(value_weight[...], rows) + value_bias).astype(bf16)
        count = q_in.shape[1]
        for start in range(0, count, span):
            at = slice(start, min(count, start + span))
            scores = dot(keys, q_in[:, at])
            before = peak_out[:, at]
            peak = jnp.maximum(before, jnp.max(scores, axis=0, keepdims=True))
            exponent = jnp.exp2((scores - peak) * factor)
            fade = jnp.exp2((before - peak) * factor)
            peak_out[:, at] = peak
            sum_out[:, at] = fade * sum_out[:, at] + jnp.sum(exponent, axis=0, keepdims=True)
            held_out[:, at] = fade * held_out[:, at] + dot(values, exponent.astype(bf16))
        return carry

    lax.fori_loop(0, blocks // 2, step, 0)


def attend_middle(key_blocks, weights, query, state):
    channels, count = query.shape
    blocks = len(key_blocks)
    total_keys = sum(k.shape[0] for k in key_blocks)
    others = (*weights, query, *state)
    return pl.pallas_call(
        functools.partial(attend_middle_kernel, blocks=blocks, span=256),
        in_specs=[pl.BlockSpec(memory_space=pl.ANY)] * blocks + [whole(a) for a in others],
        out_specs=[whole(a) for a in state],
        out_shape=[jax.ShapeDtypeStruct(a.shape, f32) for a in state],
        scratch_shapes=[
            pltpu.VMEM((blocks, *key_blocks[0].shape), bf16),
            pltpu.SemaphoreType.DMA((blocks,)),
        ],
        cost_estimate=pl.CostEstimate(
            flops=8 * total_keys * channels * (channels + count),
            transcendentals=count * total_keys,
            bytes_accessed=4 * count * channels,
        ),
    )(*key_blocks, *others)


def attend_call(key_blocks, weights, extra, first, last):
    channels = weights[1].shape[0]
    count = key_blocks[0].shape[0] if first else extra[0].shape[1]
    total_keys = sum(k.shape[0] for k in key_blocks)
    state = [
        jax.ShapeDtypeStruct((1, count), f32),
        jax.ShapeDtypeStruct((1, count), f32),
        jax.ShapeDtypeStruct((channels, count), f32),
    ]
    if last:
        out_shape = [jax.ShapeDtypeStruct((count // 2, channels), bf16)] * 2
    elif first:
        out_shape = [jax.ShapeDtypeStruct((channels, count), bf16)] + state
    else:
        out_shape = state
    flops = 4 * total_keys * channels * (channels + count)
    return pl.pallas_call(
        functools.partial(
            attend_kernel, first=first, last=last, blocks=len(key_blocks), span=256
        ),
        out_shape=out_shape,
        cost_estimate=pl.CostEstimate(
            flops=2 * flops, transcendentals=count * total_keys, bytes_accessed=4 * count * channels
        ),
    )(*key_blocks, *weights, *extra)


def settle_kernel(pieces, lines, blocked, normal, gathered, placed):
    chunks, size, channels = pieces.shape
    rows = placed.shape[0]
    width = size // rows
    gathered[...] = pieces[...].reshape(chunks * size, channels).astype(f32)
    for chunk in range(chunks):
        for row in range(rows):
            at = chunk * size + row * width
            placed[row, chunk * width : (chunk + 1) * width] = gathered[at : at + width]
    for row in range(rows):
        columns = chunks * width
        place = 0 if row == 0 else 1 if row == rows - 1 else row + 1
        span = slice(place * columns, (place + 1) * columns)
        values = placed[row].astype(bf16)
        blocked[span] = values
        normal[span] = normed(values.astype(f32), lines[4:5]).astype(bf16)


def settle(pieces, lines, rows):
    chunks, size, channels = pieces.shape
    count = chunks * size
    return pl.pallas_call(
        settle_kernel,
        out_shape=[jax.ShapeDtypeStruct((count, channels), bf16)] * 2,
        scratch_shapes=[
            pltpu.VMEM((count, channels), f32),
            pltpu.VMEM((rows, count // rows, channels), f32),
        ],
        cost_estimate=pl.CostEstimate(
            flops=10 * count * channels, transcendentals=0, bytes_accessed=6 * count * channels
        ),
    )(pieces, lines)


def attention(blocked, own, weights, q_weight, output_weight):
    rows = lax.axis_size("row")
    swap = [(i, i ^ 1) for i in range(rows)]
    onward = [(i, (i + (2 if i % 2 == 0 else -2)) % rows) for i in range(rows)]
    send = lambda block, route: lax.ppermute(block, "row", route)
    near_a = send(own, onward)
    partner = send(own, swap)
    near_b = send(partner, onward)
    query, *state = attend_call([own, partner], weights, (q_weight,), True, False)
    near_a, near_b, query = lax.optimization_barrier((near_a, near_b, query))
    far = send(near_a, onward)
    near = [near_a, near_b, send(near_a, swap), send(near_b, swap)]
    state = attend_middle(near, weights, query, state)
    far, state = lax.optimization_barrier((far, state))
    far_too = send(far, swap)
    extra = (query, *state, blocked, output_weight)
    return attend_call([far, far_too], weights, extra, False, True)


def merge_kernel(weight, out):
    row = [[weight[i, j].astype(f32) for j in range(3)] for i in range(3)]
    depth = weight.shape[2]
    for parity in range(2):
        if parity == 0:
            upper, lower = row[0], [a + b for a, b in zip(row[1], row[2])]
        else:
            upper, lower = [a + b for a, b in zip(row[0], row[1])], row[2]
        for tap, line in enumerate((upper, lower)):
            for side in range(2):
                pair = (line[0], line[1] + line[2]) if side == 0 else (line[0] + line[1], line[2])
                for place, value in enumerate(pair):
                    if side == 1:
                        value = pltpu.roll(value, 64, 1)
                    at = (2 * tap + place) * depth
                    out[parity, side, at : at + depth] = value.astype(bf16)


def merged_taps(weight):
    depth = weight.shape[2]
    padded = jnp.pad(weight, ((0, 0), (0, 0), (0, 0), (0, 256 - weight.shape[3])))
    return pl.pallas_call(
        merge_kernel,
        out_shape=jax.ShapeDtypeStruct((2, 2, 4 * depth, 256), bf16),
        cost_estimate=pl.CostEstimate(
            flops=2 * 10**9, transcendentals=0, bytes_accessed=6 * 10**6
        ),
    )(padded)


def upscale_kernel(top, edge, inner, bottom, weight, bias, out, taps, total):
    rows, columns, channels = inner.shape[0] + 2, inner.shape[1], inner.shape[2]
    at = lax.broadcasted_iota(jnp.int32, (columns, channels), 0)
    ordered = [top[0], edge[0], *(inner[k] for k in range(rows - 2)), edge[1], bottom[0]]
    for row in range(rows + 2):
        source = ordered[row]
        values = source.astype(f32)
        before = jnp.where(at > 0, pltpu.roll(values, 1, 0), 0.0)
        after = jnp.where(at < columns - 1, pltpu.roll(values, columns - 1, 0), 0.0)
        taps[row, :, :channels] = before.astype(bf16)
        taps[row, :, channels : 2 * channels] = source
        taps[row, :, 2 * channels :] = after.astype(bf16)
    for parity in range(2):
        parts = []
        for side in range(2):
            lanes = slice(side * channels, side * channels + 2 * channels)
            upper = taps[parity : parity + rows, :, lanes].reshape(rows * columns, 2 * channels)
            lower = taps[parity + 1 : parity + 1 + rows, :, lanes].reshape(
                rows * columns, 2 * channels
            )
            parts.append(
                dot(upper, weight[parity, side, : 2 * channels])
                + dot(lower, weight[parity, side, 2 * channels :])
            )
        left, right = parts
        joined = [left[:, :128], left[:, 128:] + right[:, :128], right[:, 128:]]
        for row in range(rows):
            span = slice(row * columns, (row + 1) * columns)
            start = (2 * row + parity) * columns
            for third in range(3):
                lanes = slice(third * 128, (third + 1) * 128)
                total[third, start : start + columns, :] = joined[third][span] + bias[9:10, lanes]

    def emit(column, carry):
        for third in range(3):
            rows_here = total[third, pl.ds(column, 2 * rows, stride=columns), :]
            start = pl.multiple_of(column * channels + third * 128, 128)
            out[0, :, pl.ds(start, 128)] = rows_here.astype(bf16)
        return carry

    lax.fori_loop(0, columns, emit, 0, unroll=4)


def upscale(top, edge, inner, bottom, taps, lines):
    rows, columns, channels = inner.shape[0] + 2, inner.shape[1], inner.shape[2] // 2
    width = channels // 2
    return pl.pallas_call(
        upscale_kernel,
        grid=(2,),
        in_specs=[
            pl.BlockSpec((1, columns, channels), lambda h: (0, 0, h)),
            pl.BlockSpec((2, columns, channels), lambda h: (0, 0, h)),
            pl.BlockSpec((rows - 2, columns, channels), lambda h: (0, 0, h)),
            pl.BlockSpec((1, columns, channels), lambda h: (0, 0, h)),
            whole(taps),
            whole(lines),
        ],
        out_specs=pl.BlockSpec((1, 2 * rows, columns * channels), lambda h: (h, 0, 0)),
        out_shape=jax.ShapeDtypeStruct((2, 2 * rows, columns * channels), bf16),
        scratch_shapes=[
            pltpu.VMEM((rows + 2, columns, 3 * channels), bf16),
            pltpu.VMEM((3, 2 * rows * columns, 128), f32),
        ],
        compiler_params=pltpu.CompilerParams(dimension_semantics=("arbitrary",)),
        cost_estimate=pl.CostEstimate(
            flops=2 * 2 * rows * columns * 16 * channels * width,
            transcendentals=0,
            bytes_accessed=8 * rows * columns * channels,
        ),
    )(top, edge, inner, bottom, taps, lines)


def exchange(pieces):
    return lax.all_to_all(pieces, "frame", 0, 0)


def row_rims(last, first):
    rows = lax.axis_size("row")
    top = lax.ppermute(last, "row", [(i, i + 1) for i in range(rows - 1)])
    bottom = lax.ppermute(first, "row", [(i + 1, i) for i in range(rows - 1)])
    return top, bottom


def pack_kernel(latent, out, wide, joined):
    chunks, size, channels = out.shape
    rows, columns = latent.shape[0], latent.shape[1]
    span = size // rows
    zeros = jnp.zeros((8, channels), f32)
    for row in range(rows):
        wide[row, 0:8] = zeros
        wide[row, 8 : 8 + columns] = latent[row].astype(f32)
        wide[row, 8 + columns :] = zeros
    for chunk in range(chunks):
        at = 6 + chunk * (span - 4)
        for row in range(rows):
            joined[chunk, row * span : (row + 1) * span] = wide[row, at : at + span]
        out[chunk] = joined[chunk].astype(bf16)


def pack(latent, chunks):
    rows, columns, channels = latent.shape
    size = rows * (columns // chunks + 4)
    return pl.pallas_call(
        pack_kernel,
        out_shape=jax.ShapeDtypeStruct((chunks, size, channels), bf16),
        scratch_shapes=[
            pltpu.VMEM((rows, columns + 16, channels), f32),
            pltpu.VMEM((chunks, size, channels), f32),
        ],
        cost_estimate=pl.CostEstimate(
            flops=latent.size, transcendentals=0, bytes_accessed=5 * latent.size
        ),
    )(latent)


def on_device(
    latent,
    first_gain,
    first_weight,
    first_bias,
    second_gain,
    second_weight,
    second_bias,
    attend_gain,
    project_weight,
    project_bias,
    output_weight,
    output_bias,
    temporal_weight,
    temporal_bias,
    upscale_weight,
    upscale_bias,
):
    _, rows, columns, channels = latent.shape
    chunks = lax.axis_size("frame")
    width = columns // chunks
    chunk = lax.axis_index("frame").astype(jnp.int32).reshape(1)

    turned = project_weight.T
    lines = [first_gain, first_bias, second_gain, second_bias, attend_gain]
    lines += [project_bias[k * channels : (k + 1) * channels] for k in range(3)]
    lines += [output_bias, jnp.concatenate([upscale_bias, upscale_bias])]
    prepared = (
        jnp.concatenate(lines).reshape(-1, channels),
        project_weight[:, channels : 2 * channels],
        turned[2 * channels :],
        turned[:channels],
    )
    source = exchange(pack(latent[0], chunks)).transpose(1, 0, 2)
    source = source.reshape(rows, width + 4, chunks, channels)
    last, prepared = lax.optimization_barrier((source[-1:], prepared))
    lines, key_weight, value_weight, q_weight = prepared
    top, bottom = row_rims(last, source[:1])
    second_act = conv_call(
        functools.partial(first_conv_kernel, chunks=chunks),
        (top, source, bottom, lines),
        first_weight,
        width + 2,
        chunk,
    )
    top, bottom = row_rims(second_act[-1:], second_act[:1])
    blocked = conv_call(
        second_conv_kernel, (top, second_act, bottom, source, lines), second_weight, width
    )
    blocked = blocked.reshape(rows * width, chunks, channels).transpose(1, 0, 2)
    blocked, own = settle(exchange(blocked), lines, rows)
    mixed = attention(blocked, own, (lines, key_weight, value_weight), q_weight, output_weight)
    *mixed, upscale_weight = lax.optimization_barrier((*mixed, upscale_weight))
    taps = merged_taps(upscale_weight)
    depth = temporal_weight.reshape(3 * channels, -1)

    def later(part):
        behind = [
            lax.ppermute(part, "frame", [(i, i + lag) for i in range(chunks - lag)])
            for lag in (2, 1)
        ]
        return jnp.concatenate([*behind, part], axis=-1)

    def double(stacked):
        doubled = (dot(stacked, depth) + temporal_bias).astype(bf16)
        return doubled.reshape(-1, columns, 2 * channels)

    edge, inner = later(mixed[0]), later(mixed[1])
    edge = double(edge)
    top, bottom = row_rims(edge[1:], edge[:1])
    inner = double(inner)
    return upscale(top, edge, inner, bottom, taps, lines)


def solution(mesh):
    placed = (P("frame", "row", None, None),) + (P(),) * 15
    return jax.shard_map(
        on_device, mesh=mesh, in_specs=placed, out_specs=P("frame", "row", None), check_vma=False
    )
```

```python
import functools

import jax
import jax.numpy as jnp
from jax import lax
from jax.experimental import pallas as pl
from jax.experimental.pallas import tpu as pltpu
from jax.sharding import PartitionSpec as P

epsilon = 1e-06
bf16 = jnp.bfloat16
f32 = jnp.float32


def normed(values, scaling):
    return values * lax.rsqrt(jnp.mean(values * values, axis=-1, keepdims=True) + epsilon) * scaling


def silu(values):
    return values / (1.0 + jnp.exp(-values))


def dot(a, b):
    return jnp.dot(a, b, preferred_element_type=f32)


def fill_history(taps, row, act, frames):
    count, channels = act.shape
    columns = count // frames
    frame_of = lax.broadcasted_iota(jnp.int32, act.shape, 0) & (frames - 1)
    for lag in (2, 1, 0):
        moved = act if lag == 0 else jnp.where(frame_of >= lag, pltpu.roll(act, lag, 0), 0.0)
        at = (2 - lag) * channels
        taps[row, :, :, at : at + channels] = moved.astype(bf16).reshape(columns, frames, channels)


def conv_step(taps, weight_ref, total, out_columns):
    step = pl.program_id(0)
    rows, _, frames, depth = taps.shape
    part = 0.0
    for tap in range(3):
        window = taps[pl.ds(step, rows - 2), tap : tap + out_columns]
        weight = weight_ref[:, 0, tap].reshape(depth, -1)
        part = part + dot(window.reshape(-1, depth), weight)

    @pl.when(step == 0)
    def _():
        total[...] = part

    @pl.when(step > 0)
    def _():
        total[...] += part


def first_conv_kernel(
    chunk_ref, top, mid, bottom, lines, weight, out, taps, total, *, chunks
):
    rows, columns, frames, channels = mid.shape
    out_columns = columns - 2

    @pl.when(pl.program_id(0) == 0)
    def _():
        for row in range(rows + 2):
            source = top[0] if row == 0 else bottom[0] if row == rows + 1 else mid[row - 1]
            values = source.reshape(columns * frames, channels).astype(f32)
            fill_history(taps, row, silu(normed(values, lines[0:1])), frames)

    conv_step(taps, weight, total, out_columns)

    @pl.when(pl.program_id(0) == 2)
    def _():
        chunk = chunk_ref[0]
        shape = (out_columns * frames, channels)
        column = lax.broadcasted_iota(jnp.int32, shape, 0) // frames
        inside = ((column > 0) | (chunk > 0)) & ((column < out_columns - 1) | (chunk < chunks - 1))
        for row in range(rows):
            hidden = total[row * shape[0] : (row + 1) * shape[0]] + lines[1:2]
            act = silu(normed(hidden, lines[2:3]))
            out[row] = jnp.where(inside, act, 0.0).astype(bf16).reshape(out_columns, frames, channels)


def second_conv_kernel(top, mid, bottom, latent, lines, weight, out, taps, total):
    rows, columns, frames, channels = mid.shape
    out_columns = columns - 2

    @pl.when(pl.program_id(0) == 0)
    def _():
        for row in range(rows + 2):
            source = top[0] if row == 0 else bottom[0] if row == rows + 1 else mid[row - 1]
            values = source.reshape(columns * frames, channels).astype(f32)
            fill_history(taps, row, values, frames)

    conv_step(taps, weight, total, out_columns)

    @pl.when(pl.program_id(0) == 2)
    def _():
        size = out_columns * frames
        for row in range(rows):
            hidden = total[row * size : (row + 1) * size] + lines[3:4]
            own = latent[row, 2 : 2 + out_columns].reshape(size, channels).astype(f32)
            out[row] = (own + hidden).astype(bf16).reshape(out_columns, frames, channels)


def kept(array):
    return pltpu.with_memory_space_constraint(array, pltpu.VMEM)


in_place = pl.BlockSpec(memory_space=pltpu.VMEM)


def whole(array):
    return pl.BlockSpec(array.shape, lambda *_: (0,) * array.ndim)


def tap_spec(channels):
    return pl.BlockSpec((3, 1, 3, channels, channels), lambda s: (0, s, 0, 0, 0))


def conv_call(kernel, ahead, weight, out_columns, scalar=None):
    mid = ahead[1]
    rows, columns, frames, channels = mid.shape
    scratch = [
        pltpu.VMEM((rows + 2, columns, frames, 3 * channels), bf16),
        pltpu.VMEM((rows * out_columns * frames, channels), f32),
    ]
    in_specs = [in_place if k in (0, 2) else whole(a) for k, a in enumerate(ahead)]
    in_specs += [tap_spec(channels)]
    ahead = [kept(a) if k in (0, 2) else a for k, a in enumerate(ahead)]
    operands = (*ahead, weight)
    if scalar is not None:
        operands = (scalar, *operands)
        in_specs = [pl.BlockSpec(memory_space=pltpu.SMEM)] + in_specs
    shape = (rows, out_columns, frames, channels)
    flops = 2 * 27 * rows * out_columns * frames * channels * channels
    return pl.pallas_call(
        kernel,
        grid=(3,),
        in_specs=in_specs,
        out_specs=pl.BlockSpec(shape, lambda s: (0, 0, 0, 0)),
        out_shape=jax.ShapeDtypeStruct(shape, bf16),
        scratch_shapes=scratch,
        compiler_params=pltpu.CompilerParams(dimension_semantics=("arbitrary",)),
        cost_estimate=pl.CostEstimate(
            flops=flops, transcendentals=0, bytes_accessed=2 * weight.size
        ),
    )(*operands)


def attend_kernel(*refs, first, last, blocks, span):
    refs = list(refs)
    take = lambda: refs.pop(0)
    keys_in = [take() for _ in range(blocks)]
    lines, key_weight, value_weight = take(), take(), take()
    if first:
        q_weight = take()
    else:
        q_in, peak_in, sum_in, held_in = take(), take(), take(), take()
    if last:
        source, out_weight, *outs = take(), take(), take(), take()
    else:
        if first:
            q_out = take()
        peak_out, sum_out, held_out = take(), take(), take()
    channels = key_weight.shape[0]
    factor = channels ** (-0.5) * 1.4426950408889634
    rows = jnp.concatenate([k[...] for k in keys_in], axis=0)
    keys = (dot(rows, key_weight[...]) + lines[6:7]).astype(bf16)
    values = (across(value_weight[...], rows) + upright(lines[7:8])).astype(bf16)
    count = keys_in[0].shape[0] if first else q_in.shape[1]
    for start in range(0, count, span):
        at = slice(start, min(count, start + span))
        if first:
            query = (across(q_weight[...], keys_in[0][at]) + upright(lines[5:6])).astype(bf16)
            q_out[:, at] = query
        else:
            query = q_in[:, at]
        scores = dot(keys, query)
        peak = jnp.max(scores, axis=0, keepdims=True)
        if not first:
            before = peak_in[:, at]
            peak = jnp.maximum(before, peak)
        exponent = jnp.exp2((scores - peak) * factor)
        summed = jnp.sum(exponent, axis=0, keepdims=True)
        held = dot(values, exponent.astype(bf16))
        if not first:
            fade = jnp.exp2((before - peak) * factor)
            summed = summed + fade * sum_in[:, at]
            held = held + fade * held_in[:, at]
        if last:
            attended = (held / summed).astype(bf16)
            mixed = lax.dot_general(
                attended, out_weight[...], (((0,), (0,)), ((), ())), preferred_element_type=f32
            )
            mixed = (source[at].astype(f32) + mixed + lines[8:9]).astype(bf16)
            half = outs[0].shape[0]
            for part, out in enumerate(outs):
                low, high = max(at.start, part * half), min(at.stop, (part + 1) * half)
                if low < high:
                    shift = part * half
                    out[low - shift : high - shift] = mixed[low - at.start : high - at.start]
        else:
            peak_out[:, at] = peak
            sum_out[:, at] = summed
            held_out[:, at] = held


def upright(line):
    return jnp.broadcast_to(line, (128, line.shape[1])).T[:, :1]


def across(a, b):
    return lax.dot_general(a, b, (((1,), (1,)), ((), ())), preferred_element_type=f32)


def attend_middle_kernel(
    *refs, blocks, span
):
    sources, refs = refs[:blocks], refs[blocks:]
    lines, key_weight, value_weight, q_in, peak_in, sum_in, held_in = refs[:7]
    peak_out, sum_out, held_out, arrived, done = refs[7:]
    channels = key_weight.shape[0]
    factor = channels ** (-0.5) * 1.4426950408889634
    for index, source in enumerate(sources):
        pltpu.make_async_copy(source, arrived.at[index], done.at[index]).start()
    peak_out[...] = peak_in[...]
    sum_out[...] = sum_in[...]
    held_out[...] = held_in[...]
    key_bias = lines[6:7]
    value_bias = upright(lines[7:8])

    def step(index, carry):
        for half in range(2):
            slot = 2 * index + half
            pltpu.make_async_copy(sources[0], arrived.at[slot], done.at[slot]).wait()
        rows = arrived[pl.ds(2 * index, 2)].reshape(-1, channels)
        keys = (dot(rows, key_weight[...]) + key_bias).astype(bf16)
        values = (across(value_weight[...], rows) + value_bias).astype(bf16)
        count = q_in.shape[1]
        for start in range(0, count, span):
            at = slice(start, min(count, start + span))
            scores = dot(keys, q_in[:, at])
            before = peak_out[:, at]
            peak = jnp.maximum(before, jnp.max(scores, axis=0, keepdims=True))
            exponent = jnp.exp2((scores - peak) * factor)
            fade = jnp.exp2((before - peak) * factor)
            peak_out[:, at] = peak
            sum_out[:, at] = fade * sum_out[:, at] + jnp.sum(exponent, axis=0, keepdims=True)
            held_out[:, at] = fade * held_out[:, at] + dot(values, exponent.astype(bf16))
        return carry

    lax.fori_loop(0, blocks // 2, step, 0)


def attend_middle(key_blocks, weights, query, state):
    channels, count = query.shape
    blocks = len(key_blocks)
    total_keys = sum(k.shape[0] for k in key_blocks)
    others = (*weights, query, *state)
    return pl.pallas_call(
        functools.partial(attend_middle_kernel, blocks=blocks, span=256),
        in_specs=[pl.BlockSpec(memory_space=pl.ANY)] * blocks + [whole(a) for a in others],
        out_specs=[whole(a) for a in state],
        out_shape=[jax.ShapeDtypeStruct(a.shape, f32) for a in state],
        scratch_shapes=[
            pltpu.VMEM((blocks, *key_blocks[0].shape), bf16),
            pltpu.SemaphoreType.DMA((blocks,)),
        ],
        cost_estimate=pl.CostEstimate(
            flops=8 * total_keys * channels * (channels + count),
            transcendentals=count * total_keys,
            bytes_accessed=4 * count * channels,
        ),
    )(*key_blocks, *others)


def attend_call(key_blocks, weights, extra, first, last):
    channels = weights[1].shape[0]
    count = key_blocks[0].shape[0] if first else extra[0].shape[1]
    total_keys = sum(k.shape[0] for k in key_blocks)
    state = [
        jax.ShapeDtypeStruct((1, count), f32),
        jax.ShapeDtypeStruct((1, count), f32),
        jax.ShapeDtypeStruct((channels, count), f32),
    ]
    if last:
        out_shape = [jax.ShapeDtypeStruct((count // 2, channels), bf16)] * 2
    elif first:
        out_shape = [jax.ShapeDtypeStruct((channels, count), bf16)] + state
    else:
        out_shape = state
    flops = 4 * total_keys * channels * (channels + count)
    return pl.pallas_call(
        functools.partial(
            attend_kernel, first=first, last=last, blocks=len(key_blocks), span=256
        ),
        in_specs=[in_place] * len(key_blocks) + [whole(a) for a in (*weights, *extra)],
        out_shape=out_shape,
        cost_estimate=pl.CostEstimate(
            flops=2 * flops, transcendentals=count * total_keys, bytes_accessed=4 * count * channels
        ),
    )(*[kept(k) for k in key_blocks], *weights, *extra)


def settle_kernel(pieces, lines, blocked, normal, gathered, placed):
    chunks, size, channels = pieces.shape
    rows = placed.shape[0]
    width = size // rows
    gathered[...] = pieces[...].reshape(chunks * size, channels).astype(f32)
    for chunk in range(chunks):
        for row in range(rows):
            at = chunk * size + row * width
            placed[row, chunk * width : (chunk + 1) * width] = gathered[at : at + width]
    for row in range(rows):
        columns = chunks * width
        place = 0 if row == 0 else 1 if row == rows - 1 else row + 1
        span = slice(place * columns, (place + 1) * columns)
        values = placed[row].astype(bf16)
        blocked[span] = values
        normal[span] = normed(values.astype(f32), lines[4:5]).astype(bf16)


def settle(pieces, lines, rows):
    chunks, size, channels = pieces.shape
    count = chunks * size
    return pl.pallas_call(
        settle_kernel,
        out_shape=[jax.ShapeDtypeStruct((count, channels), bf16)] * 2,
        scratch_shapes=[
            pltpu.VMEM((count, channels), f32),
            pltpu.VMEM((rows, count // rows, channels), f32),
        ],
        cost_estimate=pl.CostEstimate(
            flops=10 * count * channels, transcendentals=0, bytes_accessed=6 * count * channels
        ),
    )(pieces, lines)


def attention(blocked, own, weights, q_weight, output_weight):
    rows = lax.axis_size("row")
    swap = [(i, i ^ 1) for i in range(rows)]
    onward = [(i, (i + (2 if i % 2 == 0 else -2)) % rows) for i in range(rows)]
    send = lambda block, route: lax.ppermute(block, "row", route)
    near_a = send(own, onward)
    partner = send(own, swap)
    near_b = send(partner, onward)
    query, *state = attend_call([own, partner], weights, (q_weight,), True, False)
    near_a, near_b, query = lax.optimization_barrier((near_a, near_b, query))
    far = send(near_a, onward)
    near = [near_a, near_b, send(near_a, swap), send(near_b, swap)]
    near = [kept(block) for block in near]
    state = attend_middle(near, weights, query, state)
    far, state = lax.optimization_barrier((far, state))
    far_too = send(far, swap)
    extra = (query, *state, blocked, output_weight)
    return attend_call([far, far_too], weights, extra, False, True)


def merge_kernel(weight, out):
    row = [[weight[i, j].astype(f32) for j in range(3)] for i in range(3)]
    depth = weight.shape[2]
    for parity in range(2):
        if parity == 0:
            upper, lower = row[0], [a + b for a, b in zip(row[1], row[2])]
        else:
            upper, lower = [a + b for a, b in zip(row[0], row[1])], row[2]
        for tap, line in enumerate((upper, lower)):
            for side in range(2):
                pair = (line[0], line[1] + line[2]) if side == 0 else (line[0] + line[1], line[2])
                for place, value in enumerate(pair):
                    if side == 1:
                        value = pltpu.roll(value, 64, 1)
                    at = (2 * tap + place) * depth
                    out[parity, side, at : at + depth] = value.astype(bf16)


def merged_taps(weight):
    depth = weight.shape[2]
    padded = jnp.pad(weight, ((0, 0), (0, 0), (0, 0), (0, 256 - weight.shape[3])))
    return pl.pallas_call(
        merge_kernel,
        out_shape=jax.ShapeDtypeStruct((2, 2, 4 * depth, 256), bf16),
        cost_estimate=pl.CostEstimate(
            flops=2 * 10**9, transcendentals=0, bytes_accessed=6 * 10**6
        ),
    )(padded)


def upscale_kernel(top, edge, inner, bottom, weight, bias, out, taps, total):
    rows, columns, channels = inner.shape[0] + 2, inner.shape[1], inner.shape[2]
    at = lax.broadcasted_iota(jnp.int32, (columns, channels), 0)
    ordered = [top[0], edge[0], *(inner[k] for k in range(rows - 2)), edge[1], bottom[0]]
    for row in range(rows + 2):
        source = ordered[row]
        values = source.astype(f32)
        before = jnp.where(at > 0, pltpu.roll(values, 1, 0), 0.0)
        after = jnp.where(at < columns - 1, pltpu.roll(values, columns - 1, 0), 0.0)
        taps[row, :, :channels] = before.astype(bf16)
        taps[row, :, channels : 2 * channels] = source
        taps[row, :, 2 * channels :] = after.astype(bf16)
    for parity in range(2):
        parts = []
        for side in range(2):
            lanes = slice(side * channels, side * channels + 2 * channels)
            upper = taps[parity : parity + rows, :, lanes].reshape(rows * columns, 2 * channels)
            lower = taps[parity + 1 : parity + 1 + rows, :, lanes].reshape(
                rows * columns, 2 * channels
            )
            parts.append(
                dot(upper, weight[parity, side, : 2 * channels])
                + dot(lower, weight[parity, side, 2 * channels :])
            )
        left, right = parts
        joined = [left[:, :128], left[:, 128:] + right[:, :128], right[:, 128:]]
        for row in range(rows):
            span = slice(row * columns, (row + 1) * columns)
            start = (2 * row + parity) * columns
            for third in range(3):
                lanes = slice(third * 128, (third + 1) * 128)
                total[third, start : start + columns, :] = joined[third][span] + bias[9:10, lanes]

    def emit(column, carry):
        for third in range(3):
            rows_here = total[third, pl.ds(column, 2 * rows, stride=columns), :]
            start = pl.multiple_of(column * channels + third * 128, 128)
            out[0, :, pl.ds(start, 128)] = rows_here.astype(bf16)
        return carry

    lax.fori_loop(0, columns, emit, 0, unroll=4)


def upscale(top, edge, inner, bottom, taps, lines):
    rows, columns, channels = inner.shape[0] + 2, inner.shape[1], inner.shape[2] // 2
    width = channels // 2
    return pl.pallas_call(
        upscale_kernel,
        grid=(2,),
        in_specs=[
            pl.BlockSpec((1, columns, channels), lambda h: (0, 0, h)),
            pl.BlockSpec((2, columns, channels), lambda h: (0, 0, h)),
            pl.BlockSpec((rows - 2, columns, channels), lambda h: (0, 0, h)),
            pl.BlockSpec((1, columns, channels), lambda h: (0, 0, h)),
            whole(taps),
            whole(lines),
        ],
        out_specs=pl.BlockSpec((1, 2 * rows, columns * channels), lambda h: (h, 0, 0)),
        out_shape=jax.ShapeDtypeStruct((2, 2 * rows, columns * channels), bf16),
        scratch_shapes=[
            pltpu.VMEM((rows + 2, columns, 3 * channels), bf16),
            pltpu.VMEM((3, 2 * rows * columns, 128), f32),
        ],
        compiler_params=pltpu.CompilerParams(dimension_semantics=("arbitrary",)),
        cost_estimate=pl.CostEstimate(
            flops=2 * 2 * rows * columns * 16 * channels * width,
            transcendentals=0,
            bytes_accessed=8 * rows * columns * channels,
        ),
    )(top, edge, inner, bottom, taps, lines)


def exchange(pieces):
    return lax.all_to_all(pieces, "frame", 0, 0)


def row_rims(last, first):
    rows = lax.axis_size("row")
    top = lax.ppermute(last, "row", [(i, i + 1) for i in range(rows - 1)])
    bottom = lax.ppermute(first, "row", [(i + 1, i) for i in range(rows - 1)])
    return top, bottom


def pack_kernel(latent, out, wide, joined):
    chunks, size, channels = out.shape
    rows, columns = latent.shape[0], latent.shape[1]
    span = size // rows
    zeros = jnp.zeros((8, channels), f32)
    for row in range(rows):
        wide[row, 0:8] = zeros
        wide[row, 8 : 8 + columns] = latent[row].astype(f32)
        wide[row, 8 + columns :] = zeros
    for chunk in range(chunks):
        at = 6 + chunk * (span - 4)
        for row in range(rows):
            joined[chunk, row * span : (row + 1) * span] = wide[row, at : at + span]
        out[chunk] = joined[chunk].astype(bf16)


def pack(latent, chunks):
    rows, columns, channels = latent.shape
    size = rows * (columns // chunks + 4)
    return pl.pallas_call(
        pack_kernel,
        out_shape=jax.ShapeDtypeStruct((chunks, size, channels), bf16),
        scratch_shapes=[
            pltpu.VMEM((rows, columns + 16, channels), f32),
            pltpu.VMEM((chunks, size, channels), f32),
        ],
        cost_estimate=pl.CostEstimate(
            flops=latent.size, transcendentals=0, bytes_accessed=5 * latent.size
        ),
    )(latent)


def on_device(
    latent,
    first_gain,
    first_weight,
    first_bias,
    second_gain,
    second_weight,
    second_bias,
    attend_gain,
    project_weight,
    project_bias,
    output_weight,
    output_bias,
    temporal_weight,
    temporal_bias,
    upscale_weight,
    upscale_bias,
):
    _, rows, columns, channels = latent.shape
    chunks = lax.axis_size("frame")
    width = columns // chunks
    chunk = lax.axis_index("frame").astype(jnp.int32).reshape(1)

    turned = project_weight.T
    lines = [first_gain, first_bias, second_gain, second_bias, attend_gain]
    lines += [project_bias[k * channels : (k + 1) * channels] for k in range(3)]
    lines += [output_bias, jnp.concatenate([upscale_bias, upscale_bias])]
    prepared = (
        jnp.concatenate(lines).reshape(-1, channels),
        project_weight[:, channels : 2 * channels],
        turned[2 * channels :],
        turned[:channels],
    )
    source = exchange(pack(latent[0], chunks)).transpose(1, 0, 2)
    source = source.reshape(rows, width + 4, chunks, channels)
    last, prepared = lax.optimization_barrier((source[-1:], prepared))
    lines, key_weight, value_weight, q_weight = prepared
    top, bottom = row_rims(last, source[:1])
    second_act = conv_call(
        functools.partial(first_conv_kernel, chunks=chunks),
        (top, source, bottom, lines),
        first_weight,
        width + 2,
        chunk,
    )
    top, bottom = row_rims(second_act[-1:], second_act[:1])
    blocked = conv_call(
        second_conv_kernel, (top, second_act, bottom, source, lines), second_weight, width
    )
    blocked = blocked.reshape(rows * width, chunks, channels).transpose(1, 0, 2)
    blocked, own = settle(exchange(blocked), lines, rows)
    mixed = attention(blocked, own, (lines, key_weight, value_weight), q_weight, output_weight)
    *mixed, upscale_weight = lax.optimization_barrier((*mixed, upscale_weight))
    taps = merged_taps(upscale_weight)
    depth = temporal_weight.reshape(3 * channels, -1)

    def later(part):
        behind = [
            lax.ppermute(part, "frame", [(i, i + lag) for i in range(chunks - lag)])
            for lag in (2, 1)
        ]
        return jnp.concatenate([*behind, part], axis=-1)

    def double(stacked):
        doubled = (dot(stacked, depth) + temporal_bias).astype(bf16)
        return doubled.reshape(-1, columns, 2 * channels)

    edge, inner = later(mixed[0]), later(mixed[1])
    edge = double(edge)
    top, bottom = row_rims(edge[1:], edge[:1])
    inner = double(inner)
    return upscale(top, edge, inner, bottom, taps, lines)


def solution(mesh):
    placed = (P("frame", "row", None, None),) + (P(),) * 15
    return jax.shard_map(
        on_device, mesh=mesh, in_specs=placed, out_specs=P("frame", "row", None), check_vma=False
    )
```

```python
import functools

import jax
import jax.numpy as jnp
from jax import lax
from jax.experimental import pallas as pl
from jax.experimental.pallas import tpu as pltpu
from jax.sharding import PartitionSpec as P

epsilon = 1e-06
bf16 = jnp.bfloat16
f32 = jnp.float32


def normed(values, scaling):
    return values * lax.rsqrt(jnp.mean(values * values, axis=-1, keepdims=True) + epsilon) * scaling


def silu(values):
    return values / (1.0 + jnp.exp(-values))


def dot(a, b):
    return jnp.dot(a, b, preferred_element_type=f32)


def fill_history(taps, row, act, frames):
    count, channels = act.shape
    columns = count // frames
    frame_of = lax.broadcasted_iota(jnp.int32, act.shape, 0) & (frames - 1)
    for lag in (2, 1, 0):
        moved = act if lag == 0 else jnp.where(frame_of >= lag, pltpu.roll(act, lag, 0), 0.0)
        at = (2 - lag) * channels
        taps[row, :, :, at : at + channels] = moved.astype(bf16).reshape(columns, frames, channels)


def conv_step(taps, weight_ref, total, out_columns):
    step = pl.program_id(0)
    rows, _, frames, depth = taps.shape
    part = 0.0
    for tap in range(3):
        window = taps[pl.ds(step, rows - 2), tap : tap + out_columns]
        weight = weight_ref[:, 0, tap].reshape(depth, -1)
        part = part + dot(window.reshape(-1, depth), weight)

    @pl.when(step == 0)
    def _():
        total[...] = part

    @pl.when(step > 0)
    def _():
        total[...] += part


def first_conv_kernel(
    chunk_ref, top, mid, bottom, lines, weight, out, taps, total, *, chunks
):
    rows, columns, frames, channels = mid.shape
    out_columns = columns - 2

    @pl.when(pl.program_id(0) == 0)
    def _():
        for row in range(rows + 2):
            source = top[0] if row == 0 else bottom[0] if row == rows + 1 else mid[row - 1]
            values = source.reshape(columns * frames, channels).astype(f32)
            fill_history(taps, row, silu(normed(values, lines[0:1])), frames)

    conv_step(taps, weight, total, out_columns)

    @pl.when(pl.program_id(0) == 2)
    def _():
        chunk = chunk_ref[0]
        shape = (out_columns * frames, channels)
        column = lax.broadcasted_iota(jnp.int32, shape, 0) // frames
        inside = ((column > 0) | (chunk > 0)) & ((column < out_columns - 1) | (chunk < chunks - 1))
        for row in range(rows):
            hidden = total[row * shape[0] : (row + 1) * shape[0]] + lines[1:2]
            act = silu(normed(hidden, lines[2:3]))
            out[row] = jnp.where(inside, act, 0.0).astype(bf16).reshape(out_columns, frames, channels)


def second_conv_kernel(top, mid, bottom, latent, lines, weight, out, taps, total):
    rows, columns, frames, channels = mid.shape
    out_columns = columns - 2

    @pl.when(pl.program_id(0) == 0)
    def _():
        for row in range(rows + 2):
            source = top[0] if row == 0 else bottom[0] if row == rows + 1 else mid[row - 1]
            values = source.reshape(columns * frames, channels).astype(f32)
            fill_history(taps, row, values, frames)

    conv_step(taps, weight, total, out_columns)

    @pl.when(pl.program_id(0) == 2)
    def _():
        size = out_columns * frames
        for row in range(rows):
            hidden = total[row * size : (row + 1) * size] + lines[3:4]
            own = latent[row, 2 : 2 + out_columns].reshape(size, channels).astype(f32)
            out[row] = (own + hidden).astype(bf16).reshape(out_columns, frames, channels)


def kept(array):
    return pltpu.with_memory_space_constraint(array, pltpu.VMEM)


in_place = pl.BlockSpec(memory_space=pltpu.VMEM)


def whole(array):
    return pl.BlockSpec(array.shape, lambda *_: (0,) * array.ndim)


def tap_spec(channels):
    return pl.BlockSpec((3, 1, 3, channels, channels), lambda s: (0, s, 0, 0, 0))


def conv_call(kernel, ahead, weight, out_columns, scalar=None):
    mid = ahead[1]
    rows, columns, frames, channels = mid.shape
    scratch = [
        pltpu.VMEM((rows + 2, columns, frames, 3 * channels), bf16),
        pltpu.VMEM((rows * out_columns * frames, channels), f32),
    ]
    in_specs = [in_place if k in (0, 2) else whole(a) for k, a in enumerate(ahead)]
    in_specs += [tap_spec(channels)]
    ahead = [kept(a) if k in (0, 2) else a for k, a in enumerate(ahead)]
    operands = (*ahead, weight)
    if scalar is not None:
        operands = (scalar, *operands)
        in_specs = [pl.BlockSpec(memory_space=pltpu.SMEM)] + in_specs
    shape = (rows, out_columns, frames, channels)
    flops = 2 * 27 * rows * out_columns * frames * channels * channels
    return pl.pallas_call(
        kernel,
        grid=(3,),
        in_specs=in_specs,
        out_specs=pl.BlockSpec(shape, lambda s: (0, 0, 0, 0)),
        out_shape=jax.ShapeDtypeStruct(shape, bf16),
        scratch_shapes=scratch,
        compiler_params=pltpu.CompilerParams(dimension_semantics=("arbitrary",)),
        cost_estimate=pl.CostEstimate(
            flops=flops, transcendentals=0, bytes_accessed=2 * weight.size
        ),
    )(*operands)


def attend_kernel(*refs, first, last, blocks, span):
    refs = list(refs)
    take = lambda: refs.pop(0)
    keys_in = [take() for _ in range(blocks)]
    lines, key_weight, value_weight = take(), take(), take()
    if first:
        q_weight = take()
    else:
        q_in, peak_in, sum_in, held_in = take(), take(), take(), take()
    if last:
        source, out_weight, *outs = take(), take(), take(), take()
    else:
        if first:
            q_out = take()
        peak_out, sum_out, held_out = take(), take(), take()
    channels = key_weight.shape[0]
    factor = channels ** (-0.5) * 1.4426950408889634
    rows = jnp.concatenate([k[...] for k in keys_in], axis=0)
    keys = (dot(rows, key_weight[...]) + lines[6:7]).astype(bf16)
    values = (across(value_weight[...], rows) + upright(lines[7:8])).astype(bf16)
    count = keys_in[0].shape[0] if first else q_in.shape[1]
    for start in range(0, count, span):
        at = slice(start, min(count, start + span))
        if first:
            query = (across(q_weight[...], keys_in[0][at]) + upright(lines[5:6])).astype(bf16)
            q_out[:, at] = query
        else:
            query = q_in[:, at]
        scores = dot(keys, query)
        peak = jnp.max(scores, axis=0, keepdims=True)
        if not first:
            before = peak_in[:, at]
            peak = jnp.maximum(before, peak)
        exponent = jnp.exp2((scores - peak) * factor)
        summed = jnp.sum(exponent, axis=0, keepdims=True)
        held = dot(values, exponent.astype(bf16))
        if not first:
            fade = jnp.exp2((before - peak) * factor)
            summed = summed + fade * sum_in[:, at]
            held = held + fade * held_in[:, at]
        if last:
            attended = (held / summed).astype(bf16)
            mixed = lax.dot_general(
                attended, out_weight[...], (((0,), (0,)), ((), ())), preferred_element_type=f32
            )
            mixed = (source[at].astype(f32) + mixed + lines[8:9]).astype(bf16)
            half = outs[0].shape[0]
            for part, out in enumerate(outs):
                low, high = max(at.start, part * half), min(at.stop, (part + 1) * half)
                if low < high:
                    shift = part * half
                    out[low - shift : high - shift] = mixed[low - at.start : high - at.start]
        else:
            peak_out[:, at] = peak
            sum_out[:, at] = summed
            held_out[:, at] = held


def upright(line):
    return jnp.broadcast_to(line, (128, line.shape[1])).T[:, :1]


def across(a, b):
    return lax.dot_general(a, b, (((1,), (1,)), ((), ())), preferred_element_type=f32)


def attend_middle_kernel(
    *refs, blocks, span
):
    sources, refs = refs[:blocks], refs[blocks:]
    lines, key_weight, value_weight, q_in, peak_in, sum_in, held_in = refs[:7]
    peak_out, sum_out, held_out, arrived, done = refs[7:]
    channels = key_weight.shape[0]
    factor = channels ** (-0.5) * 1.4426950408889634
    for index, source in enumerate(sources):
        pltpu.make_async_copy(source, arrived.at[index], done.at[index]).start()
    peak_out[...] = peak_in[...]
    sum_out[...] = sum_in[...]
    held_out[...] = held_in[...]
    key_bias = lines[6:7]
    value_bias = upright(lines[7:8])

    def step(index, carry):
        for half in range(2):
            slot = 2 * index + half
            pltpu.make_async_copy(sources[0], arrived.at[slot], done.at[slot]).wait()
        rows = arrived[pl.ds(2 * index, 2)].reshape(-1, channels)
        keys = (dot(rows, key_weight[...]) + key_bias).astype(bf16)
        values = (across(value_weight[...], rows) + value_bias).astype(bf16)
        count = q_in.shape[1]
        for start in range(0, count, span):
            at = slice(start, min(count, start + span))
            scores = dot(keys, q_in[:, at])
            before = peak_out[:, at]
            peak = jnp.maximum(before, jnp.max(scores, axis=0, keepdims=True))
            exponent = jnp.exp2((scores - peak) * factor)
            fade = jnp.exp2((before - peak) * factor)
            peak_out[:, at] = peak
            sum_out[:, at] = fade * sum_out[:, at] + jnp.sum(exponent, axis=0, keepdims=True)
            held_out[:, at] = fade * held_out[:, at] + dot(values, exponent.astype(bf16))
        return carry

    lax.fori_loop(0, blocks // 2, step, 0)


def attend_middle(key_blocks, weights, query, state):
    channels, count = query.shape
    blocks = len(key_blocks)
    total_keys = sum(k.shape[0] for k in key_blocks)
    held = [kept(a) for a in (query, *state)]
    return pl.pallas_call(
        functools.partial(attend_middle_kernel, blocks=blocks, span=256),
        in_specs=[pl.BlockSpec(memory_space=pl.ANY)] * blocks
        + [whole(a) for a in weights]
        + [in_place] * len(held),
        out_specs=[in_place] * len(state),
        out_shape=[pltpu.VMEM(a.shape, f32) for a in state],
        scratch_shapes=[
            pltpu.VMEM((blocks, *key_blocks[0].shape), bf16),
            pltpu.SemaphoreType.DMA((blocks,)),
        ],
        compiler_params=pltpu.CompilerParams(vmem_limit_bytes=40 * 2**20),
        cost_estimate=pl.CostEstimate(
            flops=8 * total_keys * channels * (channels + count),
            transcendentals=count * total_keys,
            bytes_accessed=4 * count * channels,
        ),
    )(*key_blocks, *weights, *held)


def attend_call(key_blocks, weights, extra, first, last):
    channels = weights[1].shape[0]
    count = key_blocks[0].shape[0] if first else extra[0].shape[1]
    total_keys = sum(k.shape[0] for k in key_blocks)
    state = [
        pltpu.VMEM((1, count), f32),
        pltpu.VMEM((1, count), f32),
        pltpu.VMEM((channels, count), f32),
    ]
    if last:
        out_shape = [jax.ShapeDtypeStruct((count // 2, channels), bf16)] * 2
    elif first:
        out_shape = [pltpu.VMEM((channels, count), bf16)] + state
    else:
        out_shape = state
    held = 0 if first else 4
    out_specs = [whole(a) for a in out_shape] if last else [in_place] * len(out_shape)
    extra = [kept(a) if k < held else a for k, a in enumerate(extra)]
    specs = [in_place if k < held else whole(a) for k, a in enumerate(extra)]
    flops = 4 * total_keys * channels * (channels + count)
    return pl.pallas_call(
        functools.partial(
            attend_kernel, first=first, last=last, blocks=len(key_blocks), span=256
        ),
        in_specs=[in_place] * len(key_blocks) + [whole(a) for a in weights] + specs,
        out_specs=out_specs,
        out_shape=out_shape,
        compiler_params=pltpu.CompilerParams(vmem_limit_bytes=40 * 2**20),
        cost_estimate=pl.CostEstimate(
            flops=2 * flops, transcendentals=count * total_keys, bytes_accessed=4 * count * channels
        ),
    )(*[kept(k) for k in key_blocks], *weights, *extra)


def settle_kernel(pieces, lines, blocked, normal, gathered, placed):
    chunks, size, channels = pieces.shape
    rows = placed.shape[0]
    width = size // rows
    gathered[...] = pieces[...].reshape(chunks * size, channels).astype(f32)
    for chunk in range(chunks):
        for row in range(rows):
            at = chunk * size + row * width
            placed[row, chunk * width : (chunk + 1) * width] = gathered[at : at + width]
    for row in range(rows):
        columns = chunks * width
        place = 0 if row == 0 else 1 if row == rows - 1 else row + 1
        span = slice(place * columns, (place + 1) * columns)
        values = placed[row].astype(bf16)
        blocked[span] = values
        normal[span] = normed(values.astype(f32), lines[4:5]).astype(bf16)


def settle(pieces, lines, rows):
    chunks, size, channels = pieces.shape
    count = chunks * size
    return pl.pallas_call(
        settle_kernel,
        out_shape=[jax.ShapeDtypeStruct((count, channels), bf16)] * 2,
        scratch_shapes=[
            pltpu.VMEM((count, channels), f32),
            pltpu.VMEM((rows, count // rows, channels), f32),
        ],
        cost_estimate=pl.CostEstimate(
            flops=10 * count * channels, transcendentals=0, bytes_accessed=6 * count * channels
        ),
    )(pieces, lines)


def attention(blocked, own, weights, q_weight, output_weight):
    rows = lax.axis_size("row")
    swap = [(i, i ^ 1) for i in range(rows)]
    onward = [(i, (i + (2 if i % 2 == 0 else -2)) % rows) for i in range(rows)]
    send = lambda block, route: lax.ppermute(block, "row", route)
    near_a = send(own, onward)
    partner = send(own, swap)
    near_b = send(partner, onward)
    query, *state = attend_call([own, partner], weights, (q_weight,), True, False)
    near_a, near_b, query = lax.optimization_barrier((near_a, near_b, query))
    far = send(near_a, onward)
    near = [near_a, near_b, send(near_a, swap), send(near_b, swap)]
    near = [kept(block) for block in near]
    state = attend_middle(near, weights, query, state)
    far, state = lax.optimization_barrier((far, state))
    far_too = send(far, swap)
    extra = (query, *state, blocked, output_weight)
    return attend_call([far, far_too], weights, extra, False, True)


def merge_kernel(weight, out):
    row = [[weight[i, j].astype(f32) for j in range(3)] for i in range(3)]
    depth = weight.shape[2]
    for parity in range(2):
        if parity == 0:
            upper, lower = row[0], [a + b for a, b in zip(row[1], row[2])]
        else:
            upper, lower = [a + b for a, b in zip(row[0], row[1])], row[2]
        for tap, line in enumerate((upper, lower)):
            for side in range(2):
                pair = (line[0], line[1] + line[2]) if side == 0 else (line[0] + line[1], line[2])
                for place, value in enumerate(pair):
                    if side == 1:
                        value = pltpu.roll(value, 64, 1)
                    at = (2 * tap + place) * depth
                    out[parity, side, at : at + depth] = value.astype(bf16)


def merged_taps(weight):
    depth = weight.shape[2]
    padded = jnp.pad(weight, ((0, 0), (0, 0), (0, 0), (0, 256 - weight.shape[3])))
    return pl.pallas_call(
        merge_kernel,
        out_shape=jax.ShapeDtypeStruct((2, 2, 4 * depth, 256), bf16),
        cost_estimate=pl.CostEstimate(
            flops=2 * 10**9, transcendentals=0, bytes_accessed=6 * 10**6
        ),
    )(padded)


def upscale_kernel(top, edge, inner, bottom, weight, bias, out, taps, total):
    rows, columns, channels = inner.shape[0] + 2, inner.shape[1], inner.shape[2]
    at = lax.broadcasted_iota(jnp.int32, (columns, channels), 0)
    ordered = [top[0], edge[0], *(inner[k] for k in range(rows - 2)), edge[1], bottom[0]]
    for row in range(rows + 2):
        source = ordered[row]
        values = source.astype(f32)
        before = jnp.where(at > 0, pltpu.roll(values, 1, 0), 0.0)
        after = jnp.where(at < columns - 1, pltpu.roll(values, columns - 1, 0), 0.0)
        taps[row, :, :channels] = before.astype(bf16)
        taps[row, :, channels : 2 * channels] = source
        taps[row, :, 2 * channels :] = after.astype(bf16)
    for parity in range(2):
        parts = []
        for side in range(2):
            lanes = slice(side * channels, side * channels + 2 * channels)
            upper = taps[parity : parity + rows, :, lanes].reshape(rows * columns, 2 * channels)
            lower = taps[parity + 1 : parity + 1 + rows, :, lanes].reshape(
                rows * columns, 2 * channels
            )
            parts.append(
                dot(upper, weight[parity, side, : 2 * channels])
                + dot(lower, weight[parity, side, 2 * channels :])
            )
        left, right = parts
        joined = [left[:, :128], left[:, 128:] + right[:, :128], right[:, 128:]]
        for row in range(rows):
            span = slice(row * columns, (row + 1) * columns)
            start = (2 * row + parity) * columns
            for third in range(3):
                lanes = slice(third * 128, (third + 1) * 128)
                total[third, start : start + columns, :] = joined[third][span] + bias[9:10, lanes]

    def emit(column, carry):
        for third in range(3):
            rows_here = total[third, pl.ds(column, 2 * rows, stride=columns), :]
            start = pl.multiple_of(column * channels + third * 128, 128)
            out[0, :, pl.ds(start, 128)] = rows_here.astype(bf16)
        return carry

    lax.fori_loop(0, columns, emit, 0, unroll=4)


def upscale(top, edge, inner, bottom, taps, lines):
    rows, columns, channels = inner.shape[0] + 2, inner.shape[1], inner.shape[2] // 2
    width = channels // 2
    return pl.pallas_call(
        upscale_kernel,
        grid=(2,),
        in_specs=[
            pl.BlockSpec((1, columns, channels), lambda h: (0, 0, h)),
            pl.BlockSpec((2, columns, channels), lambda h: (0, 0, h)),
            pl.BlockSpec((rows - 2, columns, channels), lambda h: (0, 0, h)),
            pl.BlockSpec((1, columns, channels), lambda h: (0, 0, h)),
            whole(taps),
            whole(lines),
        ],
        out_specs=pl.BlockSpec((1, 2 * rows, columns * channels), lambda h: (h, 0, 0)),
        out_shape=jax.ShapeDtypeStruct((2, 2 * rows, columns * channels), bf16),
        scratch_shapes=[
            pltpu.VMEM((rows + 2, columns, 3 * channels), bf16),
            pltpu.VMEM((3, 2 * rows * columns, 128), f32),
        ],
        compiler_params=pltpu.CompilerParams(dimension_semantics=("arbitrary",)),
        cost_estimate=pl.CostEstimate(
            flops=2 * 2 * rows * columns * 16 * channels * width,
            transcendentals=0,
            bytes_accessed=8 * rows * columns * channels,
        ),
    )(top, edge, inner, bottom, taps, lines)


def exchange(pieces):
    return lax.all_to_all(pieces, "frame", 0, 0)


def row_rims(last, first):
    rows = lax.axis_size("row")
    top = lax.ppermute(last, "row", [(i, i + 1) for i in range(rows - 1)])
    bottom = lax.ppermute(first, "row", [(i + 1, i) for i in range(rows - 1)])
    return top, bottom


def pack_kernel(latent, out, wide, joined):
    chunks, size, channels = out.shape
    rows, columns = latent.shape[0], latent.shape[1]
    span = size // rows
    zeros = jnp.zeros((8, channels), f32)
    for row in range(rows):
        wide[row, 0:8] = zeros
        wide[row, 8 : 8 + columns] = latent[row].astype(f32)
        wide[row, 8 + columns :] = zeros
    for chunk in range(chunks):
        at = 6 + chunk * (span - 4)
        for row in range(rows):
            joined[chunk, row * span : (row + 1) * span] = wide[row, at : at + span]
        out[chunk] = joined[chunk].astype(bf16)


def pack(latent, chunks):
    rows, columns, channels = latent.shape
    size = rows * (columns // chunks + 4)
    return pl.pallas_call(
        pack_kernel,
        out_shape=jax.ShapeDtypeStruct((chunks, size, channels), bf16),
        scratch_shapes=[
            pltpu.VMEM((rows, columns + 16, channels), f32),
            pltpu.VMEM((chunks, size, channels), f32),
        ],
        cost_estimate=pl.CostEstimate(
            flops=latent.size, transcendentals=0, bytes_accessed=5 * latent.size
        ),
    )(latent)


def on_device(
    latent,
    first_gain,
    first_weight,
    first_bias,
    second_gain,
    second_weight,
    second_bias,
    attend_gain,
    project_weight,
    project_bias,
    output_weight,
    output_bias,
    temporal_weight,
    temporal_bias,
    upscale_weight,
    upscale_bias,
):
    _, rows, columns, channels = latent.shape
    chunks = lax.axis_size("frame")
    width = columns // chunks
    chunk = lax.axis_index("frame").astype(jnp.int32).reshape(1)

    turned = project_weight.T
    lines = [first_gain, first_bias, second_gain, second_bias, attend_gain]
    lines += [project_bias[k * channels : (k + 1) * channels] for k in range(3)]
    lines += [output_bias, jnp.concatenate([upscale_bias, upscale_bias])]
    prepared = (
        jnp.concatenate(lines).reshape(-1, channels),
        project_weight[:, channels : 2 * channels],
        turned[2 * channels :],
        turned[:channels],
    )
    source = exchange(pack(latent[0], chunks)).transpose(1, 0, 2)
    source = source.reshape(rows, width + 4, chunks, channels)
    last, prepared = lax.optimization_barrier((source[-1:], prepared))
    lines, key_weight, value_weight, q_weight = prepared
    top, bottom = row_rims(last, source[:1])
    second_act = conv_call(
        functools.partial(first_conv_kernel, chunks=chunks),
        (top, source, bottom, lines),
        first_weight,
        width + 2,
        chunk,
    )
    top, bottom = row_rims(second_act[-1:], second_act[:1])
    blocked = conv_call(
        second_conv_kernel, (top, second_act, bottom, source, lines), second_weight, width
    )
    blocked = blocked.reshape(rows * width, chunks, channels).transpose(1, 0, 2)
    blocked, own = settle(exchange(blocked), lines, rows)
    mixed = attention(blocked, own, (lines, key_weight, value_weight), q_weight, output_weight)
    *mixed, upscale_weight = lax.optimization_barrier((*mixed, upscale_weight))
    taps = merged_taps(upscale_weight)
    depth = temporal_weight.reshape(3 * channels, -1)

    def later(part):
        behind = [
            lax.ppermute(part, "frame", [(i, i + lag) for i in range(chunks - lag)])
            for lag in (2, 1)
        ]
        return jnp.concatenate([*behind, part], axis=-1)

    def double(stacked):
        doubled = (dot(stacked, depth) + temporal_bias).astype(bf16)
        return doubled.reshape(-1, columns, 2 * channels)

    edge, inner = later(mixed[0]), later(mixed[1])
    edge = double(edge)
    top, bottom = row_rims(edge[1:], edge[:1])
    inner = double(inner)
    return upscale(top, edge, inner, bottom, taps, lines)


def solution(mesh):
    placed = (P("frame", "row", None, None),) + (P(),) * 15
    return jax.shard_map(
        on_device, mesh=mesh, in_specs=placed, out_specs=P("frame", "row", None), check_vma=False
    )
```
